512 devices in a mesh: mem: 4 (over z_lo), gx: 16 (over y, z_hi), gy: 8 (over x, core).
Axes of the slice: x: 4, y: 4, z: 16 (z_hi: 4, z_lo: 4; z = z_hi * 4 + z_lo), core: 2. Of those that a mesh axis runs over, the one named last changes fastest.
Arguments:
- initial_states: float32 [40, 4, 128, 1024], P('mem', None, 'gx', 'gy'), may hold values from -6 to 6
- diffusivity: float32 [4, 128, 1024], P(None, 'gx', 'gy'), may hold values from 0.04 to 0.24
- ocean_mask: int32 [128, 1024], P('gx', 'gy'), may hold values 0 or 1
- obs_values: float32 [4, 16, 32, 128], P(None, None, 'gx', 'gy'), may hold values from -6 to 6
- obs_variance: float32 [4, 16, 32, 128], P(None, None, 'gx', 'gy'), may hold values from 0.25 to 4
- obs_cells: int32 [4, 16, 32, 128], P(None, None, 'gx', 'gy'), may hold values from 0 to 31
- obs_blocks: int32 [5, 32, 128], P(None, 'gx', 'gy'), may hold values from 0 to 8, as said below
Outputs:
- analysis: float32 [40, 4, 128, 1024], P('mem', None, 'gx', 'gy')
The draws below stay inside these ranges and needn't reach their ends.
Inputs may be any that keep to these rules, and one draw needn't show every extreme that they name: `ocean_mask`: 1 marks an ocean cell, 0 a land cell. `obs_cells`: the cell of the observation in its patch, row-major over 4 x 8 cells; several observations may share a cell. `obs_blocks`: for each patch, 5 different codes 3 * (r + 1) + (c + 1) of the patches at row offset r and column offset c, r and c in -1, 0, 1.
All inputs are finite; a program needn't handle non-finite values. No bound on the sum of `ocean_mask` on one device may be relied on, other than what follows from the above.
Results may differ from the reference program's by a relative error of at most 0.0003.
Values sent between devices are 32-bit elements; how exact they have to be, the bound alone decides.
A program may use at most 64 MiB of HBM per device.

```python
import math
import jax
import jax.numpy as jnp
from jax import lax

MEMBERS = 40
LEV = 4
NX = 128
NY = 1024
PSX = 4
PSY = 8
TILE_NORTHWARD_NUM = 32
TILE_EASTWARD_NUM = 128
K_OBS = 16
NSEL = 5
NS_ITERS = 7
N_GX = 16


def draw_obs_blocks(key, part):
    scores = jax.random.randint(key, (9, TILE_NORTHWARD_NUM, TILE_EASTWARD_NUM), 0, 1048576)
    ranked = scores * 16 + jnp.arange(9, dtype=jnp.int32)[:, None, None]
    ordering = jnp.argsort(ranked, axis=0)
    return ordering[:NSEL].astype(jnp.int32)


def place_ends(values, stream_key, low, high):
    extent = values.shape
    spot = [jax.random.randint(jax.random.fold_in(stream_key, axis), (), 0, extent[axis]) for axis in range(len(extent))]
    values = values.at[tuple(spot)].set(low)
    longest = extent.index(max(extent))
    spot[longest] = (spot[longest] + 1) % extent[longest]
    return values.at[tuple(spot)].set(high)


def levels(own_key, dims, shards, low, largest):
    factor_of, own = 1.0, jax.random.fold_in(own_key, 6)
    for position, parts in shards:
        steps = jnp.exp(jax.random.uniform(jax.random.fold_in(own, position), (parts,), jnp.float32, low / len(shards), largest / len(shards)))
        factor_of = factor_of * jnp.repeat(steps, dims[position] // parts).reshape([-1 if axis == position else 1 for axis in range(len(dims))])
    return factor_of


def bell_draw(own_key, extent, scale, bound, shards=(), kind=jnp.bfloat16):
    values = scale * jax.random.normal(own_key, extent, jnp.float32)
    if shards:
        values = values * levels(own_key, extent, shards, -0.22, 0.18)
    return jnp.clip(values, -bound, bound).astype(kind)


def setup_inputs(seed: int = 0) -> dict:
    arg_keys = jax.random.split(jax.random.key(seed), 8)
    return {
        "initial_states": bell_draw(arg_keys[0], (MEMBERS, LEV, NX, NY), 1.0, 6.0, ((0, 4), (2, 16), (3, 8)), jnp.float32),
        "diffusivity": jnp.clip(jnp.exp(math.log(0.24) - 1.7917595 * jax.random.uniform(arg_keys[1], (LEV, NX, NY), jnp.float32) ** levels(arg_keys[1], (LEV, NX, NY), ((1, 16), (2, 8)), -0.2, 0.2)), 0.04, 0.24),
        "ocean_mask": place_ends((jax.random.randint(arg_keys[2], (NX, NY), 0, 8) < 7).astype(jnp.int32), jax.random.fold_in(arg_keys[2], 1), 0, 1),
        "obs_values": bell_draw(arg_keys[3], (LEV, K_OBS, TILE_NORTHWARD_NUM, TILE_EASTWARD_NUM), 1.0, 6.0, ((2, 16), (3, 8)), jnp.float32),
        "obs_variance": jnp.clip(jnp.exp(math.log(4.0) - 2.7725887 * jax.random.uniform(arg_keys[4], (LEV, K_OBS, TILE_NORTHWARD_NUM, TILE_EASTWARD_NUM), jnp.float32) ** levels(arg_keys[4], (LEV, K_OBS, TILE_NORTHWARD_NUM, TILE_EASTWARD_NUM), ((2, 16), (3, 8)), -0.2, 0.2)), 0.25, 4.0),
        "obs_cells": place_ends(jax.random.randint(arg_keys[5], (LEV, K_OBS, TILE_NORTHWARD_NUM, TILE_EASTWARD_NUM), 0, PSX * PSY), jax.random.fold_in(arg_keys[5], 1), 0, (PSX * PSY) - 1).astype(jnp.int32),
        "obs_blocks": draw_obs_blocks(jax.random.fold_in(arg_keys[7], 71), 0),
    }


exact_mode = lax.Precision.HIGHEST

def advance(padded, diffusion, wet_cells):
    center = padded[..., 1:-1, 1:-1]
    beside = padded[..., 2:, 1:-1] + padded[..., :-2, 1:-1]
    beside = beside + padded[..., 1:-1, 2:] + padded[..., 1:-1, :-2]
    return wet_cells * (center + diffusion * (beside - 4.0 * center))

def divide_to_tiles(field_now, patch_rows, patch_cols):
    members = field_now.shape[0]
    reshaped = field_now.reshape(members, patch_rows, PSX, patch_cols, PSY)
    return reshaped.transpose(0, 2, 4, 1, 3).reshape(members, PSX * PSY, patch_rows, patch_cols)

def from_patches(patches, patch_rows, patch_cols):
    members = patches.shape[0]
    reshaped = patches.reshape(members, PSX, PSY, patch_rows, patch_cols)
    return reshaped.transpose(0, 3, 1, 4, 2).reshape(members, patch_rows * PSX, patch_cols * PSY)

def observe(mesh_site_group, locations):
    slot_ids = jnp.arange(mesh_site_group.shape[1]).astype(locations.dtype)
    picker = (locations[:, None] == slot_ids[None, :, None, None]).astype(jnp.float32)
    return jnp.einsum('jcab,mcab->mjab', picker, mesh_site_group, precision=exact_mode)

def obs_pack(perturbation, mean_cells, locations, values, inv_variance):
    members_obs = observe(perturbation, locations)
    mean_obs = observe(mean_cells[None], locations)[0]
    return jnp.concatenate([members_obs, (values - mean_obs)[None], inv_variance[None]], axis=0)

def ensemble_weights(obs_slab, block_codes):
    members = obs_slab.shape[0] - 2
    patch_rows = block_codes.shape[1]
    patch_cols = block_codes.shape[2]
    patch_count = patch_rows * patch_cols
    pert_list = []
    misfit_list = []
    weight_list = []
    for slot_code in range(9):
        shift_row = slot_code // 3 - 1
        shift_col = slot_code % 3 - 1
        neighbour = obs_slab[:, :, 1 + shift_row:1 + shift_row + patch_rows, 1 + shift_col:1 + shift_col + patch_cols]
        chosen = lax.optimization_barrier(jnp.sum((block_codes == slot_code).astype(jnp.float32), axis=0))
        if slot_code == 4:
            taper_weight = 1.0
        elif shift_row == 0 or shift_col == 0:
            taper_weight = 0.5
        else:
            taper_weight = 0.25
        pert_list.append(neighbour[:members].reshape(members, -1, patch_count))
        misfit_list.append(neighbour[members].reshape(-1, patch_count))
        weight_list.append((neighbour[members + 1] * (taper_weight * chosen)[None]).reshape(-1, patch_count))
    observed = jnp.concatenate(pert_list, axis=1)
    misfit = jnp.concatenate(misfit_list, axis=0)
    weight = jnp.concatenate(weight_list, axis=0)
    scaled = observed * weight[None]
    gram_matrix = jnp.einsum('kjp,mjp->kmp', scaled, observed, precision=exact_mode)
    identity = jnp.eye(members, dtype=jnp.float32)[:, :, None]
    system = identity + gram_matrix / (members - 1.0)
    trace_sum = lax.optimization_barrier(jnp.sum(system * identity, axis=(0, 1)))
    root_part = system / trace_sum
    inverse_root = jnp.broadcast_to(identity, system.shape)
    for sweep_index in range(NS_ITERS):
        product = jnp.einsum('kjp,jmp->kmp', inverse_root, root_part, precision=exact_mode)
        update = 1.5 * identity - 0.5 * product
        root_part = jnp.einsum('kjp,jmp->kmp', root_part, update, precision=exact_mode)
        inverse_root = jnp.einsum('kjp,jmp->kmp', update, inverse_root, precision=exact_mode)
    spread = inverse_root / jnp.sqrt(trace_sum)
    projected = jnp.einsum('kjp,jp->kp', scaled, misfit, precision=exact_mode) / (members - 1.0)
    partial_value = jnp.einsum('kjp,jp->kp', spread, projected, precision=exact_mode)
    centre = jnp.einsum('kjp,jp->kp', spread, partial_value, precision=exact_mode)
    return spread + centre[:, None, :]

def apply_weights(perturbation, mean_cells, transform):
    members = perturbation.shape[0]
    cell_count = perturbation.shape[1]
    flattened = perturbation.reshape(members, cell_count, -1)
    combined = jnp.einsum('kcp,kmp->mcp', flattened, transform, precision=exact_mode)
    return combined.reshape(perturbation.shape) + mean_cells[None]

def reference(initial_states, diffusivity, ocean_mask, obs_values, obs_variance, obs_cells, obs_blocks):
    wet_cells = ocean_mask.astype(jnp.float32)

    def advance_diffusion(sample_state):
        field_now = sample_state
        for sweep_index in range(2):
            padded = jnp.pad(field_now, ((0, 0), (1, 1), (1, 1)))
            field_now = advance(padded, diffusivity, wet_cells)
        return field_now
    predicted_samples = lax.map(advance_diffusion, initial_states)
    block_rows = TILE_NORTHWARD_NUM // N_GX
    results = []
    for vertical_layer_number in range(LEV):
        mesh_site_group = divide_to_tiles(predicted_samples[:, vertical_layer_number], TILE_NORTHWARD_NUM, TILE_EASTWARD_NUM)
        mean_cells = lax.optimization_barrier(jnp.mean(mesh_site_group, axis=0))
        perturbation = mesh_site_group - mean_cells[None]
        packed = obs_pack(perturbation, mean_cells, obs_cells[vertical_layer_number], obs_values[vertical_layer_number], 1.0 / obs_variance[vertical_layer_number])
        padded = jnp.pad(packed, ((0, 0), (0, 0), (1, 1), (1, 1)))

        def one_block(block_index):
            first_row = block_index * block_rows
            obs_slab = lax.dynamic_slice_in_dim(padded, first_row, block_rows + 2, 2)
            block_codes = lax.dynamic_slice_in_dim(obs_blocks, first_row, block_rows, 1)
            local_pert = lax.dynamic_slice_in_dim(perturbation, first_row, block_rows, 2)
            local_mean = lax.dynamic_slice_in_dim(mean_cells, first_row, block_rows, 1)
            transform = ensemble_weights(obs_slab, block_codes)
            return apply_weights(local_pert, local_mean, transform)
        blocks = lax.map(one_block, jnp.arange(N_GX).astype(jnp.int32))
        analysed = jnp.moveaxis(blocks, 0, 2).reshape(MEMBERS, PSX * PSY, TILE_NORTHWARD_NUM, TILE_EASTWARD_NUM)
        results.append(from_patches(analysed, TILE_NORTHWARD_NUM, TILE_EASTWARD_NUM))
    return jnp.stack(results, axis=1)
```

```python
import jax
import jax.numpy as jnp
from jax import lax
from jax.experimental import pallas as pl
from jax.experimental.pallas import tpu as pltpu
from jax.sharding import PartitionSpec as P

MESH = pl.DeviceIdType.MESH
F32 = jnp.float32
NS_ITERS = 7
LEVELS = 4
OWN = 10
MEMBERS = 40
OBS = 16
AUX = 32
NEED = ((16, 64), (0, 80), (0, 64))


def gather_kernel(n_gx, n_gy, x_ref, aux_ref, g_ref, a_ref, ssem, rsem, asem, arsem, fsem, frsem, lsem):
    mem, gx, gy = lax.axis_index("mem"), lax.axis_index("gx"), lax.axis_index("gy")
    rows = (lax.rem(gx + n_gx - 1, n_gx), gx, lax.rem(gx + 1, n_gx))
    sides = (lax.rem(gy + n_gy - 1, n_gy), lax.rem(gy + 1, n_gy))
    there = [lax.rem(mem + o, LEVELS) for o in range(LEVELS)]
    back = [lax.rem(mem + LEVELS - o, LEVELS) for o in range(LEVELS)]

    barrier = pltpu.get_barrier_semaphore()
    count = 0
    for d in range(3):
        for o in range(LEVELS):
            if d == 1 and o == 0:
                continue
            pl.semaphore_signal(barrier, inc=1, device_id=(there[o], rows[d], gy), device_id_type=MESH)
            count += 1
    for side in sides:
        pl.semaphore_signal(barrier, inc=1, device_id=(mem, gx, side), device_id_type=MESH)
        count += 1

    own = pltpu.make_async_copy(x_ref.at[mem], g_ref.at[1, 1, mem], lsem.at[0])
    own_aux = pltpu.make_async_copy(aux_ref, a_ref.at[1, 1], lsem.at[1])
    own.start()
    own_aux.start()
    pl.semaphore_wait(barrier, count)

    sends = []

    def forward(source, dg, slot, part, index):
        for e, side in enumerate(sides):
            h = 2 if e == 0 else 0
            dst = a_ref.at[h, dg] if slot is None else g_ref.at[h, dg, slot, part]
            copy = pltpu.make_async_remote_copy(
                src_ref=source, dst_ref=dst, send_sem=fsem.at[e, dg, index], recv_sem=frsem.at[h // 2, dg, index],
                device_id=(mem, gx, side), device_id_type=MESH)
            copy.start()
            sends.append(copy)

    def scatter(d, o):
        part = pl.ds(*NEED[2 - d])
        copy = pltpu.make_async_remote_copy(
            src_ref=x_ref.at[there[o], part], dst_ref=g_ref.at[1, 2 - d, mem, part],
            send_sem=ssem.at[d, o], recv_sem=rsem.at[2 - d, o],
            device_id=(there[o], rows[d], gy), device_id_type=MESH)
        copy.start()
        sends.append(copy)

    for d in (0, 2):
        copy = pltpu.make_async_remote_copy(
            src_ref=aux_ref, dst_ref=a_ref.at[1, 2 - d], send_sem=asem.at[d], recv_sem=arsem.at[2 - d],
            device_id=(mem, rows[d], gy), device_id_type=MESH)
        copy.start()
        sends.append(copy)
    for o in range(LEVELS):
        scatter(0, o)
        scatter(2, o)
    for o in range(1, LEVELS):
        scatter(1, o)
    forward(aux_ref, 1, None, None, LEVELS)
    forward(x_ref.at[mem], 1, mem, pl.ds(0, 80), 0)

    def arrival(dg, o, source):
        part = pl.ds(*NEED[dg])
        return pltpu.make_async_remote_copy(
            src_ref=x_ref.at[0, part], dst_ref=g_ref.at[1, dg, source, part],
            send_sem=ssem.at[dg, o], recv_sem=rsem.at[dg, o],
            device_id=(mem, rows[dg], gy), device_id_type=MESH)

    for dg, o in [(1, 1), (1, 3), (1, 2)]:
        arrival(dg, o, back[o]).wait_recv()
        forward(g_ref.at[1, dg, back[o], pl.ds(*NEED[dg])], dg, back[o], pl.ds(*NEED[dg]), o)
    for dg in (0, 2):
        pltpu.make_async_remote_copy(
            src_ref=aux_ref, dst_ref=a_ref.at[1, dg], send_sem=asem.at[dg], recv_sem=arsem.at[dg],
            device_id=(mem, rows[dg], gy), device_id_type=MESH).wait_recv()
        forward(a_ref.at[1, dg], dg, None, None, LEVELS)
    for o in range(LEVELS):
        for dg in (0, 2):
            arrival(dg, o, back[o]).wait_recv()
            forward(g_ref.at[1, dg, back[o], pl.ds(*NEED[dg])], dg, back[o], pl.ds(*NEED[dg]), o)
    for h in (0, 2):
        for dg in range(3):
            for o in range(LEVELS):
                part = pl.ds(*NEED[dg])
                pltpu.make_async_remote_copy(
                    src_ref=x_ref.at[0, part], dst_ref=g_ref.at[h, dg, back[o], part],
                    send_sem=fsem.at[0, dg, o], recv_sem=frsem.at[h // 2, dg, o],
                    device_id=(mem, gx, sides[0]), device_id_type=MESH).wait_recv()
            pltpu.make_async_remote_copy(
                src_ref=aux_ref, dst_ref=a_ref.at[h, dg],
                send_sem=fsem.at[0, dg, LEVELS], recv_sem=frsem.at[h // 2, dg, LEVELS],
                device_id=(mem, gx, sides[0]), device_id_type=MESH).wait_recv()
    for copy in sends:
        copy.wait_send()
    own.wait()
    own_aux.wait()


def split(x):
    high = x.astype(jnp.bfloat16).astype(F32)
    return high, x - high


def mxu(a, b):
    return lax.dot_general(a, b, (((1,), (0,)), ((), ())), preferred_element_type=F32)


def mxu_nt(a, b):
    return lax.dot_general(a, b, (((1,), (1,)), ((), ())), preferred_element_type=F32)


def iota(shape, axis):
    return lax.broadcasted_iota(jnp.int32, shape, axis)


def block_of(lane):
    return jnp.where(lane < 40, 0, jnp.where(lane < 80, 1, jnp.where(lane < 120, 2, 3)))


def three_high(value, block):
    parts = [jnp.where(block == i, value, 0.0) for i in range(3)]
    return jnp.concatenate(parts + [jnp.zeros((8, value.shape[1]), F32)], axis=0)


def compute_kernel(n_gx, n_gy, g_ref, a_ref, ob_ref, out_ref, f0, f1, dif, wet, pt, mean, slab, wc, gram, tr, tv, ps, zs):
    gx, gy = lax.axis_index("gx"), lax.axis_index("gy")
    up = jnp.where(gx > 0, 1.0, 0.0).astype(F32)
    down = jnp.where(gx < n_gx - 1, 1.0, 0.0).astype(F32)
    west = jnp.where(gy > 0, 1.0, 0.0).astype(F32)
    east = jnp.where(gy < n_gy - 1, 1.0, 0.0).astype(F32)
    in_grid = (up, jnp.float32(1.0), down)
    lane1 = iota((1, 128), 1)
    beside = jnp.where(lane1 < 64, east, west)

    def both(h_of, dg):
        own = h_of(1) * in_grid[dg]
        side = jnp.where(lane1 < 64, h_of(2), h_of(0)) * (beside * in_grid[dg])
        return own, side

    for t in range(20):
        dg, r = (0, t + 2) if t < 6 else (1, t - 6) if t < 14 else (2, t - 14)
        main = 8 * r if r < 2 else 16 + 8 * r
        rest = 16 + 2 * r
        for s in range(LEVELS):
            own, side = both(lambda h: g_ref[h, dg, s, main:main + 8, :], dg)
            f0[t, 8 * s:8 * s + 8, 0:128] = own
            f0[t, 8 * s:8 * s + 8, 128:256] = side
            own, side = both(lambda h: g_ref[h, dg, s, rest:rest + 2, :], dg)
            f0[t, 32 + 2 * s:34 + 2 * s, 0:128] = own
            f0[t, 32 + 2 * s:34 + 2 * s, 128:256] = side
        own, side = both(lambda h: a_ref[h, dg, r:r + 1, :], dg)
        dif[t, :, 0:128] = own
        dif[t, :, 128:256] = side
        own, side = both(lambda h: a_ref[h, dg, 8 + r:9 + r, :], dg)
        wet[t, :, 0:128] = own
        wet[t, :, 128:256] = side

    def advance(src, t):
        c = src[t]
        around = src[t + 1] + src[t - 1]
        around = around + pltpu.roll(c, 255, 1) + pltpu.roll(c, 1, 1)
        return wet[t] * (c + dif[t] * (around - 4.0 * c))

    def first(t, carry):
        f1[t] = advance(f0, t)
        return carry

    lax.fori_loop(1, 19, first, 0)

    def second(p, carry):
        for r in range(4):
            value = advance(f1, 2 + 4 * p + r)
            m = jnp.sum(value, axis=0, keepdims=True) / MEMBERS
            q = value - m
            tail = jnp.where(iota((8, 256), 0) == 0, m, 0.0)
            for k in range(2):
                at = 512 * k + 128 * r
                pt[p, 0:40, at:at + 128] = q[:, 128 * k:128 * k + 128]
                pt[p, 40:48, at:at + 128] = tail[:, 128 * k:128 * k + 128]
            mean[p, :, 128 * r:128 * r + 128] = m[:, 0:128]
        return carry

    lax.fori_loop(0, 4, second, 0)

    lane2 = iota((1, 256), 1)
    inverse_of = []
    for p in range(4):
        dg, a = ((0, 1), (1, 0), (1, 1), (2, 0))[p]

        def rows_of(kind):
            at = 16 + (a * 3 + kind) * 2
            own = jnp.concatenate([a_ref[1, dg, at:at + 1, :], a_ref[1, dg, at + 1:at + 2, :]], axis=1)
            return own, jnp.where(lane1 < 64, a_ref[2, dg, at:at + 1, :], a_ref[0, dg, at + 1:at + 2, :])

        value, variance, cell = rows_of(0), rows_of(1), rows_of(2)
        found = []
        for k, (lane, shift) in enumerate(((lane2, 0), (lane1, jnp.where(lane1 < 64, 0, 64)))):
            c = cell[k].astype(jnp.int32)
            target = (c >> 3) * 128 + ((lane >> 4) << 3) + (c & 7) + shift
            hot = jnp.where(iota((512, lane.shape[1]), 0) == target, 1.0, 0.0).astype(F32)
            high, low = split(pt[p, :, 512 * k:512 * k + 512])
            both_parts = mxu(jnp.concatenate([high, low], axis=0), hot)
            found.append(both_parts[0:48] + both_parts[48:96])
        whole = jnp.concatenate(found, axis=1)
        values = jnp.concatenate(value, axis=1)
        tail = whole[40:48]
        tail = jnp.where(iota((8, 384), 0) == 0, values - tail, 0.0)
        slab[p, 0:40, :] = whole[0:40]
        slab[p, 40:48, :] = tail
        inside = jnp.concatenate([jnp.ones((1, 256), F32), beside], axis=1) * in_grid[dg]
        inverse_of.append(inside / jnp.concatenate(variance, axis=1))

    third = lax.rem(iota((1, 384), 1) >> 4, 3)
    for a in range(2):
        for r in range(3):
            near = []
            for c in range(3):
                code = 3 * r + c
                taper = 1.0 if code == 4 else 0.5 if (r == 1 or c == 1) else 0.25
                chosen = jnp.zeros((1, 256), F32)
                for s in range(5):
                    at = (s * 2 + a) * 2
                    blocks = jnp.concatenate([ob_ref[at:at + 1, :], ob_ref[at + 1:at + 2, :]], axis=1)
                    chosen = chosen + jnp.where(blocks == code, taper, 0.0)
                chosen = jnp.concatenate([chosen, jnp.zeros((1, 128), F32)], axis=1)
                near.append(pltpu.roll(chosen, (16 * (c - 1)) % 384, 1) if c != 1 else chosen)
            for i in range(3):
                which = lax.rem(third + 4 - i, 3)
                w = jnp.where(which == 0, near[0], jnp.where(which == 1, near[1], near[2]))
                wc[a, 3 * r + i:3 * r + i + 1, :] = w * inverse_of[a + r]

    slot = lane1 >> 4
    block = block_of(lane1)
    own_slot = [(slot >= i) & (slot <= i + 2) for i in range(3)]
    diagonal = (lane1 - 40 * block == iota((40, 128), 0)) & (lane1 < 120)
    for g in range(6):
        turn = (16 - 48 * g) % 384

        def window(x):
            return (pltpu.roll(x, turn, 1) if turn else x)[:, 0:128]

        parts = [window(slab[p]) for p in range(4)]
        for a in range(2):
            weights = window(wc[a])
            left = jnp.concatenate(parts[a:a + 3], axis=1)
            right = []
            for i in range(3):
                right.append(jnp.concatenate([
                    parts[a + r][0:40] * jnp.where(own_slot[i], weights[3 * r + i:3 * r + i + 1], 0.0)
                    for r in range(3)], axis=1))
            right.append(jnp.zeros((8, 384), F32))
            right = jnp.concatenate(right, axis=0)
            lh, ll = split(left)
            rh, rl = split(right)
            o = mxu_nt(jnp.concatenate([lh, ll], axis=0), jnp.concatenate([rh, rl], axis=0))
            o = o[0:48] + o[48:96]
            o = o[:, 0:128] + o[:, 128:256]
            system = jnp.where(diagonal, 1.0, 0.0) + o[0:40] / (MEMBERS - 1.0)
            n = a * 6 + g
            gram[n, 0:40, :] = system
            gram[n, 40:48, :] = o[40:48] / (MEMBERS - 1.0)
            tr[n:n + 1, :] = jnp.sum(jnp.where(diagonal, system, 0.0), axis=0, keepdims=True)

    rows = tr[...]
    sums = [jnp.sum(jnp.where(block == i, rows, 0.0), axis=1, keepdims=True) for i in range(3)]
    tv[...] = jnp.where(block == 0, sums[0], jnp.where(block == 1, sums[1], sums[2]))
    for n in range(12):
        ps[n] = gram[n, 0:40, :] / tv[n:n + 1, :]
        zs[n] = jnp.where(diagonal, 1.0, 0.0)

    wide = jnp.concatenate([block, block], axis=1)

    def sweep(step, carry):
        for n in range(12):
            p, z = ps[n], zs[n]
            pair = jnp.concatenate(split(p), axis=1)
            stacked = three_high(pair, wide)
            right = jnp.concatenate([stacked, stacked], axis=0)
            o = mxu(jnp.concatenate([pair, jnp.concatenate(split(z), axis=1)], axis=0), right)
            o = o[:, 0:128] + o[:, 128:256]
            zs[n] = 1.5 * z - 0.5 * o[40:80]
            q = 1.5 * p - 0.5 * o[0:40]
            o = mxu(jnp.concatenate(split(q), axis=1), right)
            ps[n] = 1.5 * q - 0.5 * (o[:, 0:128] + o[:, 128:256])
        return carry

    lax.fori_loop(0, NS_ITERS - 1, sweep, 0)

    ones = jnp.where((block_of(iota((128, 128), 0)) == block) & (lane1 < 120), 1.0, 0.0).astype(F32)
    ones = jnp.concatenate([ones, ones], axis=0)
    patch = lax.rem(iota((1, 512), 1), 128) >> 3
    for a in range(2):
        total = jnp.zeros((40, 512), F32)
        ph, plow = split(pt[a + 1, 0:40, 0:512])
        for g in range(6):
            n = a * 6 + g
            p, z = ps[n], zs[n]
            pair = jnp.concatenate(split(p), axis=1)
            stacked = three_high(pair, wide)
            o = mxu(jnp.concatenate(split(z), axis=1), jnp.concatenate([stacked, stacked], axis=0))
            z = 1.5 * z - 0.5 * (o[:, 0:128] + o[:, 128:256])
            spread = z / jnp.sqrt(tv[n:n + 1, :])
            partial = mxu(jnp.concatenate(split(spread * gram[n, 40:41, :]), axis=1), ones)
            centre = jnp.sum(spread * partial, axis=0, keepdims=True)
            th, tl = split(spread + centre)
            high = three_high_by(ph, patch, 3 * g)
            low = three_high_by(plow, patch, 3 * g)
            total = total + mxu(jnp.concatenate([th, tl, th], axis=1), jnp.concatenate([high, high, low], axis=0))
        total = total + mean[a + 1]
        for r in range(4):
            value = total[:, 128 * r:128 * r + 128]
            for s in range(LEVELS):
                out_ref[s, 0:8, 4 * a + r, :] = value[8 * s:8 * s + 8]
                out_ref[s, 8:10, 4 * a + r, :] = value[32 + 2 * s:34 + 2 * s]


def three_high_by(value, patch, first):
    parts = [jnp.where(patch == first + i, value, 0.0) for i in range(3)]
    return jnp.concatenate(parts + [jnp.zeros((8, value.shape[1]), F32)], axis=0)


def return_kernel(y_ref, out_ref, ssem, rsem, lsem):
    mem, gx, gy = lax.axis_index("mem"), lax.axis_index("gx"), lax.axis_index("gy")
    there = [lax.rem(mem + o, LEVELS) for o in range(LEVELS)]
    back = [lax.rem(mem + LEVELS - o, LEVELS) for o in range(LEVELS)]
    barrier = pltpu.get_barrier_semaphore()
    for o in range(1, LEVELS):
        pl.semaphore_signal(barrier, inc=1, device_id=(there[o], gx, gy), device_id_type=MESH)
    own = pltpu.make_async_copy(y_ref.at[mem], out_ref.at[mem], lsem.at[0])
    own.start()
    pl.semaphore_wait(barrier, LEVELS - 1)
    sends = []
    for o in range(1, LEVELS):
        copy = pltpu.make_async_remote_copy(
            src_ref=y_ref.at[there[o]], dst_ref=out_ref.at[mem], send_sem=ssem.at[o], recv_sem=rsem.at[o],
            device_id=(there[o], gx, gy), device_id_type=MESH)
        copy.start()
        sends.append(copy)
    for o in range(1, LEVELS):
        pltpu.make_async_remote_copy(
            src_ref=y_ref.at[0], dst_ref=out_ref.at[back[o]], send_sem=ssem.at[o], recv_sem=rsem.at[o],
            device_id=(there[o], gx, gy), device_id_type=MESH).wait_recv()
    for copy in sends:
        copy.wait_send()
    own.wait()


def prepare(initial_states, diffusivity, ocean_mask, obs_values, obs_variance, obs_cells, obs_blocks):
    x = initial_states.transpose(1, 2, 0, 3)
    main = x[:, :, :8]
    chunks = jnp.concatenate([
        main[:, :2].reshape(LEVELS, 16, 128), x[:, :, 8:].reshape(LEVELS, 16, 128),
        main[:, 2:].reshape(LEVELS, 48, 128)], axis=1)
    level = lax.axis_index("mem")

    def lanes(v):
        v = lax.dynamic_index_in_dim(v, level, 0, keepdims=False).astype(F32)
        return v.transpose(1, 2, 0).reshape(2, 2, 128)

    obs = jnp.stack([lanes(obs_values), lanes(obs_variance), lanes(obs_cells)], axis=1).reshape(12, 128)
    aux = jnp.concatenate([
        lax.dynamic_index_in_dim(diffusivity, level, 0, keepdims=False), ocean_mask.astype(F32), obs,
        jnp.zeros((4, 128), F32)], axis=0)
    blocks = jnp.broadcast_to(obs_blocks[:, :, :, None], obs_blocks.shape + (OBS,)).reshape(20, 128)
    return chunks, aux, blocks


def compute_call(n_gx, n_gy, gathered, aux, blocks, **kw):
    vmem = pl.BlockSpec(memory_space=pltpu.VMEM)
    scratch = [
        pltpu.VMEM((20, 40, 256), F32), pltpu.VMEM((20, 40, 256), F32),
        pltpu.VMEM((20, 1, 256), F32), pltpu.VMEM((20, 1, 256), F32),
        pltpu.VMEM((4, 48, 1024), F32), pltpu.VMEM((4, 1, 512), F32),
        pltpu.VMEM((4, 48, 384), F32), pltpu.VMEM((2, 9, 384), F32),
        pltpu.VMEM((12, 48, 128), F32), pltpu.VMEM((12, 128), F32), pltpu.VMEM((12, 128), F32),
        pltpu.VMEM((12, 40, 128), F32), pltpu.VMEM((12, 40, 128), F32)]

    def body(*refs):
        compute_kernel(n_gx, n_gy, *refs)

    return pl.pallas_call(
        body, out_shape=jax.ShapeDtypeStruct((LEVELS, OWN, 8, 128), F32),
        in_specs=[vmem] * 3, out_specs=vmem, scratch_shapes=scratch, name="analyse", **kw)(gathered, aux, blocks)


def solution(mesh):
    n_gx, n_gy = mesh.shape["gx"], mesh.shape["gy"]
    vmem = pl.BlockSpec(memory_space=pltpu.VMEM)

    def local(*args):
        chunks, aux, blocks = prepare(*args)
        dma = pltpu.SemaphoreType.DMA

        def gather_body(*refs):
            gather_kernel(n_gx, n_gy, *refs)

        gathered, aux_all = pl.pallas_call(
            gather_body,
            out_shape=(jax.ShapeDtypeStruct((3, 3, LEVELS, 80, 128), F32), jax.ShapeDtypeStruct((3, 3, AUX, 128), F32)),
            in_specs=[vmem] * 2, out_specs=(vmem, vmem),
            scratch_shapes=[dma((3, LEVELS)), dma((3, LEVELS)), dma((3,)), dma((3,)),
                            dma((2, 3, LEVELS + 1)), dma((2, 3, LEVELS + 1)), dma((2,))],
            compiler_params=pltpu.CompilerParams(collective_id=0, has_side_effects=True),
            name="gather")(chunks, aux)
        analysed = compute_call(n_gx, n_gy, gathered, aux_all, blocks)
        out = pl.pallas_call(
            return_kernel, out_shape=jax.ShapeDtypeStruct((LEVELS, OWN, 8, 128), F32),
            in_specs=[vmem], out_specs=vmem,
            scratch_shapes=[dma((LEVELS,)), dma((LEVELS,)), dma((1,))],
            compiler_params=pltpu.CompilerParams(collective_id=1, has_side_effects=True),
            name="give_back")(analysed)
        return out.transpose(1, 0, 2, 3)

    return jax.shard_map(
        local,
        mesh=mesh,
        in_specs=(
            P("mem", None, "gx", "gy"),
            P(None, "gx", "gy"),
            P("gx", "gy"),
            P(None, None, "gx", "gy"),
            P(None, None, "gx", "gy"),
            P(None, None, "gx", "gy"),
            P(None, "gx", "gy"),
        ),
        out_specs=P("mem", None, "gx", "gy"),
        check_vma=False,
    )
```

```python
import jax
import jax.numpy as jnp
from jax import lax
from jax.experimental import pallas as pl
from jax.experimental.pallas import tpu as pltpu
from jax.sharding import PartitionSpec as P

MESH = pl.DeviceIdType.MESH
F32 = jnp.float32
NS_ITERS = 7
LEVELS = 4
OWN = 10
MEMBERS = 40
OBS = 16
AUX = 32
NEED = ((16, 64), (0, 80), (0, 64))


def neighbours(n_gx, n_gy):
    mem, gx, gy = lax.axis_index("mem"), lax.axis_index("gx"), lax.axis_index("gy")
    rows = (lax.rem(gx + n_gx - 1, n_gx), gx, lax.rem(gx + 1, n_gx))
    sides = (lax.rem(gy + n_gy - 1, n_gy), lax.rem(gy + 1, n_gy))
    there = [lax.rem(mem + o, LEVELS) for o in range(LEVELS)]
    back = [lax.rem(mem + LEVELS - o, LEVELS) for o in range(LEVELS)]
    return mem, gx, gy, rows, sides, there, back


def prepare(level, x_ref, dif_ref, mask_ref, val_ref, var_ref, cell_ref, blk_ref, xs, aux, ob):
    flat = x_ref.reshape(OWN * LEVELS * 8, 128)
    for k in range(LEVELS):
        for r in range(8):
            main = 8 * r if r < 2 else 16 + 8 * r
            xs[k, main:main + 8, :] = flat[pl.ds(k * 8 + r, 8, stride=32), :]
            xs[k, 16 + 2 * r:18 + 2 * r, :] = flat[pl.ds(256 + k * 8 + r, 2, stride=32), :]
    aux[0:8, :] = dif_ref[level]
    aux[8:16, :] = mask_ref[...].astype(F32)
    spread_out = jnp.where(iota((16, 256), 0) == iota((16, 256), 1) >> 4, 1.0, 0.0).astype(F32)
    kinds = [ref[level].astype(F32) for ref in (val_ref, var_ref, cell_ref)]
    stacked = jnp.concatenate([kinds[k][:, a, :] for a in range(2) for k in range(3)], axis=0)
    wide = lax.dot_general(stacked, spread_out, (((1,), (0,)), ((), ())), precision=lax.Precision.HIGHEST,
                           preferred_element_type=F32)
    mine = iota((16, 256), 0) == (iota((16, 256), 1) & 15)
    for n in range(6):
        row = jnp.sum(jnp.where(mine, wide[16 * n:16 * n + 16], 0.0), axis=0, keepdims=True)
        aux[16 + 2 * n:17 + 2 * n, :] = row[:, 0:128]
        aux[17 + 2 * n:18 + 2 * n, :] = row[:, 128:256]
    aux[28:32, :] = jnp.zeros((4, 128), F32)
    blocks = blk_ref[...].astype(F32)
    blocks = jnp.concatenate([blocks[:, a, :] for a in range(2)] + [jnp.zeros((6, 16), F32)], axis=0)
    ob[...] = mxu(blocks, spread_out)


def cycle_kernel(n_gx, n_gy, x_any, dif_any, mask_any, val_any, var_any, cell_any, blk_any, out_ref,
                 x_ref, dif_ref, mask_ref, val_ref, var_ref, cell_ref, blk_ref, xs, aux, ob, g_ref, a_ref, y_ref, *rest):
    scratch, (ssem, rsem, asem, arsem, fsem, frsem, lsem, bsem, brsem) = rest[:-9], rest[-9:]
    mem, gx, gy, rows, sides, there, back = neighbours(n_gx, n_gy)

    barrier = pltpu.get_barrier_semaphore()
    count = 0
    for d in range(3):
        for o in range(LEVELS):
            if d == 1 and o == 0:
                continue
            pl.semaphore_signal(barrier, inc=1, device_id=(there[o], rows[d], gy), device_id_type=MESH)
            count += 1
    for side in sides:
        pl.semaphore_signal(barrier, inc=1, device_id=(mem, gx, side), device_id_type=MESH)
        count += 1

    loads = [pltpu.make_async_copy(src, dst, lsem.at[n]) for n, (src, dst) in enumerate((
        (x_any, x_ref), (dif_any, dif_ref), (mask_any, mask_ref), (val_any, val_ref), (var_any, var_ref),
        (cell_any, cell_ref), (blk_any, blk_ref)))]
    for load in loads:
        load.start()
    for load in loads:
        load.wait()
    prepare(mem, x_ref, dif_ref, mask_ref, val_ref, var_ref, cell_ref, blk_ref, xs, aux, ob)
    pl.semaphore_wait(barrier, count)

    sends = []

    def forward(source, dg, slot, part, index):
        for e, side in enumerate(sides):
            h = 2 if e == 0 else 0
            dst = a_ref.at[h, dg] if slot is None else g_ref.at[h, dg, slot, part]
            copy = pltpu.make_async_remote_copy(
                src_ref=source, dst_ref=dst, send_sem=fsem.at[e, dg, index], recv_sem=frsem.at[h // 2, dg, index],
                device_id=(mem, gx, side), device_id_type=MESH)
            copy.start()
            sends.append(copy)

    def scatter(d, o):
        part = pl.ds(*NEED[2 - d])
        copy = pltpu.make_async_remote_copy(
            src_ref=xs.at[there[o], part], dst_ref=g_ref.at[1, 2 - d, mem, part],
            send_sem=ssem.at[d, o], recv_sem=rsem.at[2 - d, o],
            device_id=(there[o], rows[d], gy), device_id_type=MESH)
        copy.start()
        sends.append(copy)

    for d in (0, 2):
        copy = pltpu.make_async_remote_copy(
            src_ref=aux, dst_ref=a_ref.at[1, 2 - d], send_sem=asem.at[d], recv_sem=arsem.at[2 - d],
            device_id=(mem, rows[d], gy), device_id_type=MESH)
        copy.start()
        sends.append(copy)
    for o in range(LEVELS):
        scatter(0, o)
        scatter(2, o)
    for o in range(1, LEVELS):
        scatter(1, o)
    forward(aux, 1, None, None, LEVELS)
    forward(xs.at[mem], 1, mem, pl.ds(0, 80), 0)
    g_ref[1, 1, mem] = xs[mem]
    a_ref[1, 1] = aux[...]

    def arrival(dg, o):
        part = pl.ds(*NEED[dg])
        pltpu.make_async_remote_copy(
            src_ref=xs.at[0, part], dst_ref=g_ref.at[1, dg, back[o], part],
            send_sem=ssem.at[dg, o], recv_sem=rsem.at[dg, o],
            device_id=(mem, rows[dg], gy), device_id_type=MESH).wait_recv()
        forward(g_ref.at[1, dg, back[o], part], dg, back[o], part, o)

    for o in (1, 3, 2):
        arrival(1, o)
    for dg in (0, 2):
        pltpu.make_async_remote_copy(
            src_ref=aux, dst_ref=a_ref.at[1, dg], send_sem=asem.at[dg], recv_sem=arsem.at[dg],
            device_id=(mem, rows[dg], gy), device_id_type=MESH).wait_recv()
        forward(a_ref.at[1, dg], dg, None, None, LEVELS)
    for o in range(LEVELS):
        for dg in (0, 2):
            arrival(dg, o)
    for h in (0, 2):
        for dg in range(3):
            for o in range(LEVELS):
                part = pl.ds(*NEED[dg])
                pltpu.make_async_remote_copy(
                    src_ref=xs.at[0, part], dst_ref=g_ref.at[h, dg, back[o], part],
                    send_sem=fsem.at[0, dg, o], recv_sem=frsem.at[h // 2, dg, o],
                    device_id=(mem, gx, sides[0]), device_id_type=MESH).wait_recv()
            pltpu.make_async_remote_copy(
                src_ref=aux, dst_ref=a_ref.at[h, dg],
                send_sem=fsem.at[0, dg, LEVELS], recv_sem=frsem.at[h // 2, dg, LEVELS],
                device_id=(mem, gx, sides[0]), device_id_type=MESH).wait_recv()

    compute_kernel(n_gx, n_gy, g_ref, a_ref, ob, y_ref, *scratch)

    for o in range(1, LEVELS):
        copy = pltpu.make_async_remote_copy(
            src_ref=y_ref.at[there[o]], dst_ref=out_ref.at[:, mem], send_sem=bsem.at[o], recv_sem=brsem.at[o],
            device_id=(there[o], gx, gy), device_id_type=MESH)
        copy.start()
        sends.append(copy)
    out_ref[:, mem] = y_ref[mem]
    for o in range(1, LEVELS):
        pltpu.make_async_remote_copy(
            src_ref=y_ref.at[0], dst_ref=out_ref.at[:, back[o]], send_sem=bsem.at[o], recv_sem=brsem.at[o],
            device_id=(there[o], gx, gy), device_id_type=MESH).wait_recv()
    for copy in sends:
        copy.wait_send()


def split(x):
    high = x.astype(jnp.bfloat16).astype(F32)
    return high, x - high


def mxu(a, b):
    return lax.dot_general(a, b, (((1,), (0,)), ((), ())), preferred_element_type=F32)


def mxu_nt(a, b):
    return lax.dot_general(a, b, (((1,), (1,)), ((), ())), preferred_element_type=F32)


def iota(shape, axis):
    return lax.broadcasted_iota(jnp.int32, shape, axis)


def block_of(lane):
    return jnp.where(lane < 40, 0, jnp.where(lane < 80, 1, jnp.where(lane < 120, 2, 3)))


def three_high(value, block):
    parts = [jnp.where(block == i, value, 0.0) for i in range(3)]
    return jnp.concatenate(parts + [jnp.zeros((8, value.shape[1]), F32)], axis=0)


def compute_kernel(n_gx, n_gy, g_ref, a_ref, ob_ref, out_ref, f0, f1, dif, wet, pt, mean, slab, wc, gram, tr, tv, ps, zs):
    gx, gy = lax.axis_index("gx"), lax.axis_index("gy")
    up = jnp.where(gx > 0, 1.0, 0.0).astype(F32)
    down = jnp.where(gx < n_gx - 1, 1.0, 0.0).astype(F32)
    west = jnp.where(gy > 0, 1.0, 0.0).astype(F32)
    east = jnp.where(gy < n_gy - 1, 1.0, 0.0).astype(F32)
    in_grid = (up, jnp.float32(1.0), down)
    lane1 = iota((1, 128), 1)
    beside = jnp.where(lane1 < 64, east, west)

    def both(h_of, dg):
        own = h_of(1) * in_grid[dg]
        side = jnp.where(lane1 < 64, h_of(2), h_of(0)) * (beside * in_grid[dg])
        return own, side

    for t in range(20):
        dg, r = (0, t + 2) if t < 6 else (1, t - 6) if t < 14 else (2, t - 14)
        main = 8 * r if r < 2 else 16 + 8 * r
        rest = 16 + 2 * r
        for s in range(LEVELS):
            own, side = both(lambda h: g_ref[h, dg, s, main:main + 8, :], dg)
            f0[t, 8 * s:8 * s + 8, 0:128] = own
            f0[t, 8 * s:8 * s + 8, 128:256] = side
            own, side = both(lambda h: g_ref[h, dg, s, rest:rest + 2, :], dg)
            f0[t, 32 + 2 * s:34 + 2 * s, 0:128] = own
            f0[t, 32 + 2 * s:34 + 2 * s, 128:256] = side
        own, side = both(lambda h: a_ref[h, dg, r:r + 1, :], dg)
        dif[t, :, 0:128] = own
        dif[t, :, 128:256] = side
        own, side = both(lambda h: a_ref[h, dg, 8 + r:9 + r, :], dg)
        wet[t, :, 0:128] = own
        wet[t, :, 128:256] = side

    def advance(src, t):
        c = src[t]
        around = src[t + 1] + src[t - 1]
        around = around + pltpu.roll(c, 255, 1) + pltpu.roll(c, 1, 1)
        return wet[t] * (c + dif[t] * (around - 4.0 * c))

    def first(t, carry):
        f1[t] = advance(f0, t)
        return carry

    lax.fori_loop(1, 19, first, 0)

    def second(p, carry):
        for r in range(4):
            value = advance(f1, 2 + 4 * p + r)
            m = jnp.sum(value, axis=0, keepdims=True) / MEMBERS
            q = value - m
            tail = jnp.where(iota((8, 256), 0) == 0, m, 0.0)
            for k in range(2):
                at = 512 * k + 128 * r
                pt[p, 0:40, at:at + 128] = q[:, 128 * k:128 * k + 128]
                pt[p, 40:48, at:at + 128] = tail[:, 128 * k:128 * k + 128]
            mean[p, :, 128 * r:128 * r + 128] = m[:, 0:128]
        return carry

    lax.fori_loop(0, 4, second, 0)

    lane2 = iota((1, 256), 1)
    inverse_of = []
    for p in range(4):
        dg, a = ((0, 1), (1, 0), (1, 1), (2, 0))[p]

        def rows_of(kind):
            at = 16 + (a * 3 + kind) * 2
            own = jnp.concatenate([a_ref[1, dg, at:at + 1, :], a_ref[1, dg, at + 1:at + 2, :]], axis=1)
            return own, jnp.where(lane1 < 64, a_ref[2, dg, at:at + 1, :], a_ref[0, dg, at + 1:at + 2, :])

        value, variance, cell = rows_of(0), rows_of(1), rows_of(2)
        found = []
        for k, (lane, shift) in enumerate(((lane2, 0), (lane1, jnp.where(lane1 < 64, 0, 64)))):
            c = cell[k].astype(jnp.int32)
            target = (c >> 3) * 128 + ((lane >> 4) << 3) + (c & 7) + shift
            hot = jnp.where(iota((512, lane.shape[1]), 0) == target, 1.0, 0.0).astype(F32)
            high, low = split(pt[p, :, 512 * k:512 * k + 512])
            both_parts = mxu(jnp.concatenate([high, low], axis=0), hot)
            found.append(both_parts[0:48] + both_parts[48:96])
        whole = jnp.concatenate(found, axis=1)
        values = jnp.concatenate(value, axis=1)
        tail = whole[40:48]
        tail = jnp.where(iota((8, 384), 0) == 0, values - tail, 0.0)
        slab[p, 0:40, :] = whole[0:40]
        slab[p, 40:48, :] = tail
        inside = jnp.concatenate([jnp.ones((1, 256), F32), beside], axis=1) * in_grid[dg]
        inverse_of.append(inside / jnp.concatenate(variance, axis=1))

    third = lax.rem(iota((1, 384), 1) >> 4, 3)
    for a in range(2):
        for r in range(3):
            near = []
            for c in range(3):
                code = 3 * r + c
                taper = 1.0 if code == 4 else 0.5 if (r == 1 or c == 1) else 0.25
                chosen = jnp.zeros((1, 256), F32)
                for s in range(5):
                    blocks = ob_ref[5 * a + s:5 * a + s + 1, :]
                    chosen = chosen + jnp.where(blocks == code, taper, 0.0)
                chosen = jnp.concatenate([chosen, jnp.zeros((1, 128), F32)], axis=1)
                near.append(pltpu.roll(chosen, (16 * (c - 1)) % 384, 1) if c != 1 else chosen)
            for i in range(3):
                which = lax.rem(third + 4 - i, 3)
                w = jnp.where(which == 0, near[0], jnp.where(which == 1, near[1], near[2]))
                wc[a, 3 * r + i:3 * r + i + 1, :] = w * inverse_of[a + r]

    slot = lane1 >> 4
    block = block_of(lane1)
    own_slot = [(slot >= i) & (slot <= i + 2) for i in range(3)]
    diagonal = (lane1 - 40 * block == iota((40, 128), 0)) & (lane1 < 120)
    for g in range(6):
        turn = (16 - 48 * g) % 384

        def window(x):
            return (pltpu.roll(x, turn, 1) if turn else x)[:, 0:128]

        parts = [window(slab[p]) for p in range(4)]
        for a in range(2):
            weights = window(wc[a])
            left = jnp.concatenate(parts[a:a + 3], axis=1)
            right = []
            for i in range(3):
                right.append(jnp.concatenate([
                    parts[a + r][0:40] * jnp.where(own_slot[i], weights[3 * r + i:3 * r + i + 1], 0.0)
                    for r in range(3)], axis=1))
            right.append(jnp.zeros((8, 384), F32))
            right = jnp.concatenate(right, axis=0)
            lh, ll = split(left)
            rh, rl = split(right)
            o = mxu_nt(jnp.concatenate([lh, ll], axis=0), jnp.concatenate([rh, rl], axis=0))
            o = o[0:48] + o[48:96]
            o = o[:, 0:128] + o[:, 128:256]
            system = jnp.where(diagonal, 1.0, 0.0) + o[0:40] / (MEMBERS - 1.0)
            n = a * 6 + g
            gram[n, 0:40, :] = system
            gram[n, 40:48, :] = o[40:48] / (MEMBERS - 1.0)
            tr[n:n + 1, :] = jnp.sum(jnp.where(diagonal, system, 0.0), axis=0, keepdims=True)

    rows = tr[...]
    sums = [jnp.sum(jnp.where(block == i, rows, 0.0), axis=1, keepdims=True) for i in range(3)]
    tv[...] = jnp.where(block == 0, sums[0], jnp.where(block == 1, sums[1], sums[2]))
    for n in range(12):
        ps[n] = gram[n, 0:40, :] / tv[n:n + 1, :]
        zs[n] = jnp.where(diagonal, 1.0, 0.0)

    wide = jnp.concatenate([block, block], axis=1)

    def sweep(step, carry):
        for n in range(12):
            p, z = ps[n], zs[n]
            pair = jnp.concatenate(split(p), axis=1)
            stacked = three_high(pair, wide)
            right = jnp.concatenate([stacked, stacked], axis=0)
            o = mxu(jnp.concatenate([pair, jnp.concatenate(split(z), axis=1)], axis=0), right)
            o = o[:, 0:128] + o[:, 128:256]
            zs[n] = 1.5 * z - 0.5 * o[40:80]
            q = 1.5 * p - 0.5 * o[0:40]
            o = mxu(jnp.concatenate(split(q), axis=1), right)
            ps[n] = 1.5 * q - 0.5 * (o[:, 0:128] + o[:, 128:256])
        return carry

    lax.fori_loop(0, NS_ITERS - 1, sweep, 0)

    ones = jnp.where((block_of(iota((128, 128), 0)) == block) & (lane1 < 120), 1.0, 0.0).astype(F32)
    ones = jnp.concatenate([ones, ones], axis=0)
    patch = lax.rem(iota((1, 512), 1), 128) >> 3
    for a in range(2):
        total = jnp.zeros((40, 512), F32)
        ph, plow = split(pt[a + 1, 0:40, 0:512])
        for g in range(6):
            n = a * 6 + g
            p, z = ps[n], zs[n]
            pair = jnp.concatenate(split(p), axis=1)
            stacked = three_high(pair, wide)
            o = mxu(jnp.concatenate(split(z), axis=1), jnp.concatenate([stacked, stacked], axis=0))
            z = 1.5 * z - 0.5 * (o[:, 0:128] + o[:, 128:256])
            spread = z / jnp.sqrt(tv[n:n + 1, :])
            partial = mxu(jnp.concatenate(split(spread * gram[n, 40:41, :]), axis=1), ones)
            centre = jnp.sum(spread * partial, axis=0, keepdims=True)
            th, tl = split(spread + centre)
            high = three_high_by(ph, patch, 3 * g)
            low = three_high_by(plow, patch, 3 * g)
            total = total + mxu(jnp.concatenate([th, tl, th], axis=1), jnp.concatenate([high, high, low], axis=0))
        total = total + mean[a + 1]
        flat = out_ref.reshape(MEMBERS * 8, 128)
        for r in range(4):
            value = total[:, 128 * r:128 * r + 128]
            for s in range(LEVELS):
                flat[pl.ds(80 * s + 4 * a + r, 8, stride=8), :] = value[8 * s:8 * s + 8]
                flat[pl.ds(80 * s + 64 + 4 * a + r, 2, stride=8), :] = value[32 + 2 * s:34 + 2 * s]


def three_high_by(value, patch, first):
    parts = [jnp.where(patch == first + i, value, 0.0) for i in range(3)]
    return jnp.concatenate(parts + [jnp.zeros((8, value.shape[1]), F32)], axis=0)


def scratch_of():
    return [
        pltpu.VMEM((20, 40, 256), F32), pltpu.VMEM((20, 40, 256), F32),
        pltpu.VMEM((20, 1, 256), F32), pltpu.VMEM((20, 1, 256), F32),
        pltpu.VMEM((4, 48, 1024), F32), pltpu.VMEM((4, 1, 512), F32),
        pltpu.VMEM((4, 48, 384), F32), pltpu.VMEM((2, 9, 384), F32),
        pltpu.VMEM((12, 48, 128), F32), pltpu.VMEM((12, 128), F32), pltpu.VMEM((12, 128), F32),
        pltpu.VMEM((12, 40, 128), F32), pltpu.VMEM((12, 40, 128), F32)]


def solution(mesh):
    n_gx, n_gy = mesh.shape["gx"], mesh.shape["gy"]
    dma = pltpu.SemaphoreType.DMA

    def local(*args):
        def body(*refs):
            cycle_kernel(n_gx, n_gy, *refs)

        return pl.pallas_call(
            body, out_shape=jax.ShapeDtypeStruct((OWN, LEVELS, 8, 128), F32),
            in_specs=[pl.BlockSpec(memory_space=pl.ANY)] * 7, out_specs=pl.BlockSpec(memory_space=pltpu.VMEM),
            scratch_shapes=[pltpu.VMEM(a.shape, a.dtype) for a in args] + [
                pltpu.VMEM((LEVELS, 80, 128), F32), pltpu.VMEM((AUX, 128), F32), pltpu.VMEM((16, 256), F32),
                pltpu.VMEM((3, 3, LEVELS, 80, 128), F32), pltpu.VMEM((3, 3, AUX, 128), F32),
                pltpu.VMEM((LEVELS, OWN, 8, 128), F32)] + scratch_of() + [
                dma((3, LEVELS)), dma((3, LEVELS)), dma((3,)), dma((3,)),
                dma((2, 3, LEVELS + 1)), dma((2, 3, LEVELS + 1)), dma((7,)), dma((LEVELS,)), dma((LEVELS,))],
            compiler_params=pltpu.CompilerParams(collective_id=0, has_side_effects=True),
            name="cycle")(*args)

    return jax.shard_map(
        local,
        mesh=mesh,
        in_specs=(
            P("mem", None, "gx", "gy"),
            P(None, "gx", "gy"),
            P("gx", "gy"),
            P(None, None, "gx", "gy"),
            P(None, None, "gx", "gy"),
            P(None, None, "gx", "gy"),
            P(None, "gx", "gy"),
        ),
        out_specs=P("mem", None, "gx", "gy"),
        check_vma=False,
    )
```

```python
import jax
import jax.numpy as jnp
from jax import lax
from jax.experimental import pallas as pl
from jax.experimental.pallas import tpu as pltpu
from jax.sharding import PartitionSpec as P

MESH = pl.DeviceIdType.MESH
F32 = jnp.float32
NS_ITERS = 7
LEVELS = 4
OWN = 10
MEMBERS = 40
OBS = 16
AUX = 32
NEED = ((16, 64), (0, 80), (0, 64))


def neighbours(n_gx, n_gy):
    mem, gx, gy = lax.axis_index("mem"), lax.axis_index("gx"), lax.axis_index("gy")
    rows = (lax.rem(gx + n_gx - 1, n_gx), gx, lax.rem(gx + 1, n_gx))
    sides = (lax.rem(gy + n_gy - 1, n_gy), lax.rem(gy + 1, n_gy))
    there = [lax.rem(mem + o, LEVELS) for o in range(LEVELS)]
    back = [lax.rem(mem + LEVELS - o, LEVELS) for o in range(LEVELS)]
    return mem, gx, gy, rows, sides, there, back


def prepare(level, x_ref, dif_ref, mask_ref, val_ref, var_ref, cell_ref, blk_ref, xs, aux, ob):
    flat = x_ref.reshape(OWN * LEVELS * 8, 128)
    for k in range(LEVELS):
        for r in range(8):
            main = 8 * r if r < 2 else 16 + 8 * r
            xs[k, main:main + 8, :] = flat[pl.ds(k * 8 + r, 8, stride=32), :]
            xs[k, 16 + 2 * r:18 + 2 * r, :] = flat[pl.ds(256 + k * 8 + r, 2, stride=32), :]
    aux[0:8, :] = dif_ref[level]
    aux[8:16, :] = mask_ref[...].astype(F32)
    spread_out = jnp.where(iota((16, 256), 0) == iota((16, 256), 1) >> 4, 1.0, 0.0).astype(F32)
    kinds = [ref[level].astype(F32) for ref in (val_ref, var_ref, cell_ref)]
    stacked = jnp.concatenate([kinds[k][:, a, :] for a in range(2) for k in range(3)], axis=0)
    wide = lax.dot_general(stacked, spread_out, (((1,), (0,)), ((), ())), precision=lax.Precision.HIGHEST,
                           preferred_element_type=F32)
    mine = iota((16, 256), 0) == (iota((16, 256), 1) & 15)
    for n in range(6):
        row = jnp.sum(jnp.where(mine, wide[16 * n:16 * n + 16], 0.0), axis=0, keepdims=True)
        aux[16 + 2 * n:17 + 2 * n, :] = row[:, 0:128]
        aux[17 + 2 * n:18 + 2 * n, :] = row[:, 128:256]
    aux[28:32, :] = jnp.zeros((4, 128), F32)
    blocks = blk_ref[...].astype(F32)
    blocks = jnp.concatenate([blocks[:, a, :] for a in range(2)] + [jnp.zeros((6, 16), F32)], axis=0)
    ob[...] = mxu(blocks, spread_out)


def cycle_kernel(n_gx, n_gy, x_any, dif_any, mask_any, val_any, var_any, cell_any, blk_any, out_ref,
                 x_ref, dif_ref, mask_ref, val_ref, var_ref, cell_ref, blk_ref, xs, aux, ob, g_ref, a_ref, y_ref, *rest):
    scratch, (ssem, rsem, asem, arsem, fsem, frsem, lsem, bsem, brsem) = rest[:-9], rest[-9:]
    mem, gx, gy, rows, sides, there, back = neighbours(n_gx, n_gy)

    in_rows = (gx > 0, None, gx < n_gx - 1)
    in_sides = (gy > 0, gy < n_gy - 1)

    def when(*conditions):
        known = [c for c in conditions if c is not None]
        if not known:
            return lambda f: f()
        return pl.when(known[0] if len(known) == 1 else known[0] & known[1])

    barrier = pltpu.get_barrier_semaphore()
    count = LEVELS - 1
    for d in range(3):
        @when(in_rows[d])
        def _():
            for o in range(1 if d == 1 else 0, LEVELS):
                pl.semaphore_signal(barrier, inc=1, device_id=(there[o], rows[d], gy), device_id_type=MESH)
        if d != 1:
            count = count + jnp.where(in_rows[d], LEVELS, 0)
    for e in range(2):
        @when(in_sides[e])
        def _():
            pl.semaphore_signal(barrier, inc=1, device_id=(mem, gx, sides[e]), device_id_type=MESH)
        count = count + jnp.where(in_sides[e], 1, 0)

    loads = [pltpu.make_async_copy(src, dst, lsem.at[n]) for n, (src, dst) in enumerate((
        (x_any, x_ref), (dif_any, dif_ref), (mask_any, mask_ref), (val_any, val_ref), (var_any, var_ref),
        (cell_any, cell_ref), (blk_any, blk_ref)))]
    for load in loads:
        load.start()
    for load in loads:
        load.wait()
    prepare(mem, x_ref, dif_ref, mask_ref, val_ref, var_ref, cell_ref, blk_ref, xs, aux, ob)
    for dg in (0, 2):
        @when(~in_rows[dg])
        def _():
            for h in range(3):
                g_ref[h, dg] = jnp.zeros((LEVELS, 80, 128), F32)
                a_ref[h, dg] = jnp.ones((AUX, 128), F32)
    for h in (0, 2):
        @when(~in_sides[h // 2])
        def _():
            g_ref[h] = jnp.zeros((3, LEVELS, 80, 128), F32)
            a_ref[h] = jnp.ones((3, AUX, 128), F32)
    pl.semaphore_wait(barrier, count)

    sends = []

    def start(copy, *conditions):
        when(*conditions)(copy.start)
        sends.append((copy, conditions))

    def forward(source, dg, slot, part, index):
        for e, side in enumerate(sides):
            h = 2 if e == 0 else 0
            dst = a_ref.at[h, dg] if slot is None else g_ref.at[h, dg, slot, part]
            start(pltpu.make_async_remote_copy(
                src_ref=source, dst_ref=dst, send_sem=fsem.at[e, dg, index], recv_sem=frsem.at[h // 2, dg, index],
                device_id=(mem, gx, side), device_id_type=MESH), in_rows[dg], in_sides[e])

    def scatter(d, o):
        part = pl.ds(*NEED[2 - d])
        start(pltpu.make_async_remote_copy(
            src_ref=xs.at[there[o], part], dst_ref=g_ref.at[1, 2 - d, mem, part],
            send_sem=ssem.at[d, o], recv_sem=rsem.at[2 - d, o],
            device_id=(there[o], rows[d], gy), device_id_type=MESH), in_rows[d])

    def scatter_aux(d):
        start(pltpu.make_async_remote_copy(
            src_ref=aux, dst_ref=a_ref.at[1, 2 - d], send_sem=asem.at[d], recv_sem=arsem.at[2 - d],
            device_id=(mem, rows[d], gy), device_id_type=MESH), in_rows[d])

    forward(aux, 1, None, None, LEVELS)
    forward(xs.at[mem], 1, mem, pl.ds(0, 80), 0)
    for o in range(1, LEVELS):
        scatter(1, o)
    for d in (0, 2):
        scatter_aux(d)
    for o in range(LEVELS):
        scatter(0, o)
        scatter(2, o)
    g_ref[1, 1, mem] = xs[mem]
    a_ref[1, 1] = aux[...]

    def arrival(dg, o):
        part = pl.ds(*NEED[dg])

        @when(in_rows[dg])
        def _():
            pltpu.make_async_remote_copy(
                src_ref=xs.at[0, part], dst_ref=g_ref.at[1, dg, back[o], part],
                send_sem=ssem.at[dg, o], recv_sem=rsem.at[dg, o],
                device_id=(mem, rows[dg], gy), device_id_type=MESH).wait_recv()
        forward(g_ref.at[1, dg, back[o], part], dg, back[o], part, o)

    for o in (1, 3, 2):
        arrival(1, o)
    for dg in (0, 2):
        @when(in_rows[dg])
        def _():
            pltpu.make_async_remote_copy(
                src_ref=aux, dst_ref=a_ref.at[1, dg], send_sem=asem.at[dg], recv_sem=arsem.at[dg],
                device_id=(mem, rows[dg], gy), device_id_type=MESH).wait_recv()
        forward(a_ref.at[1, dg], dg, None, None, LEVELS)
    for o in range(LEVELS):
        for dg in (0, 2):
            arrival(dg, o)
    for h in (0, 2):
        for dg in (1, 0, 2):
            @when(in_sides[h // 2], in_rows[dg])
            def _():
                for o in range(LEVELS):
                    part = pl.ds(*NEED[dg])
                    pltpu.make_async_remote_copy(
                        src_ref=xs.at[0, part], dst_ref=g_ref.at[h, dg, back[o], part],
                        send_sem=fsem.at[0, dg, o], recv_sem=frsem.at[h // 2, dg, o],
                        device_id=(mem, gx, sides[0]), device_id_type=MESH).wait_recv()
                pltpu.make_async_remote_copy(
                    src_ref=aux, dst_ref=a_ref.at[h, dg],
                    send_sem=fsem.at[0, dg, LEVELS], recv_sem=frsem.at[h // 2, dg, LEVELS],
                    device_id=(mem, gx, sides[0]), device_id_type=MESH).wait_recv()

    compute_kernel(n_gx, n_gy, g_ref, a_ref, ob, y_ref, *scratch)

    for o in range(1, LEVELS):
        start(pltpu.make_async_remote_copy(
            src_ref=y_ref.at[there[o]], dst_ref=out_ref.at[:, mem], send_sem=bsem.at[o], recv_sem=brsem.at[o],
            device_id=(there[o], gx, gy), device_id_type=MESH))
    out_ref[:, mem] = y_ref[mem]
    for o in range(1, LEVELS):
        pltpu.make_async_remote_copy(
            src_ref=y_ref.at[0], dst_ref=out_ref.at[:, back[o]], send_sem=bsem.at[o], recv_sem=brsem.at[o],
            device_id=(there[o], gx, gy), device_id_type=MESH).wait_recv()
    for copy, conditions in sends:
        when(*conditions)(copy.wait_send)


def split(x):
    high = x.astype(jnp.bfloat16).astype(F32)
    return high, x - high


def mxu(a, b):
    return lax.dot_general(a, b, (((1,), (0,)), ((), ())), preferred_element_type=F32)


def mxu_nt(a, b):
    return lax.dot_general(a, b, (((1,), (1,)), ((), ())), preferred_element_type=F32)


def iota(shape, axis):
    return lax.broadcasted_iota(jnp.int32, shape, axis)


def block_of(lane):
    return jnp.where(lane < 40, 0, jnp.where(lane < 80, 1, jnp.where(lane < 120, 2, 3)))


def three_high(value, block):
    parts = [jnp.where(block == i, value, 0.0) for i in range(3)]
    return jnp.concatenate(parts + [jnp.zeros((8, value.shape[1]), F32)], axis=0)


def compute_kernel(n_gx, n_gy, g_ref, a_ref, ob_ref, out_ref, f0, f1, dif, wet, pt, mean, slab, wc, gram, tr, tv, ps, zs):
    gx, gy = lax.axis_index("gx"), lax.axis_index("gy")
    up = jnp.where(gx > 0, 1.0, 0.0).astype(F32)
    down = jnp.where(gx < n_gx - 1, 1.0, 0.0).astype(F32)
    west = jnp.where(gy > 0, 1.0, 0.0).astype(F32)
    east = jnp.where(gy < n_gy - 1, 1.0, 0.0).astype(F32)
    in_grid = (up, jnp.float32(1.0), down)
    lane1 = iota((1, 128), 1)
    beside = jnp.where(lane1 < 64, east, west)

    def both(h_of, dg):
        own = h_of(1) * in_grid[dg]
        side = jnp.where(lane1 < 64, h_of(2), h_of(0)) * (beside * in_grid[dg])
        return own, side

    for t in range(20):
        dg, r = (0, t + 2) if t < 6 else (1, t - 6) if t < 14 else (2, t - 14)
        main = 8 * r if r < 2 else 16 + 8 * r
        rest = 16 + 2 * r
        for s in range(LEVELS):
            own, side = both(lambda h: g_ref[h, dg, s, main:main + 8, :], dg)
            f0[t, 8 * s:8 * s + 8, 0:128] = own
            f0[t, 8 * s:8 * s + 8, 128:256] = side
            own, side = both(lambda h: g_ref[h, dg, s, rest:rest + 2, :], dg)
            f0[t, 32 + 2 * s:34 + 2 * s, 0:128] = own
            f0[t, 32 + 2 * s:34 + 2 * s, 128:256] = side
        own, side = both(lambda h: a_ref[h, dg, r:r + 1, :], dg)
        dif[t, :, 0:128] = own
        dif[t, :, 128:256] = side
        own, side = both(lambda h: a_ref[h, dg, 8 + r:9 + r, :], dg)
        wet[t, :, 0:128] = own
        wet[t, :, 128:256] = side

    def advance(src, t):
        c = src[t]
        around = src[t + 1] + src[t - 1]
        around = around + pltpu.roll(c, 255, 1) + pltpu.roll(c, 1, 1)
        return wet[t] * (c + dif[t] * (around - 4.0 * c))

    def first(t, carry):
        f1[t] = advance(f0, t)
        return carry

    lax.fori_loop(1, 19, first, 0)

    def second(p, carry):
        for r in range(4):
            value = advance(f1, 2 + 4 * p + r)
            m = jnp.sum(value, axis=0, keepdims=True) / MEMBERS
            q = value - m
            tail = jnp.where(iota((8, 256), 0) == 0, m, 0.0)
            for k in range(2):
                at = 512 * k + 128 * r
                pt[p, 0:40, at:at + 128] = q[:, 128 * k:128 * k + 128]
                pt[p, 40:48, at:at + 128] = tail[:, 128 * k:128 * k + 128]
            mean[p, :, 128 * r:128 * r + 128] = m[:, 0:128]
        return carry

    lax.fori_loop(0, 4, second, 0)

    lane2 = iota((1, 256), 1)
    inverse_of = []
    for p in range(4):
        dg, a = ((0, 1), (1, 0), (1, 1), (2, 0))[p]

        def rows_of(kind):
            at = 16 + (a * 3 + kind) * 2
            own = jnp.concatenate([a_ref[1, dg, at:at + 1, :], a_ref[1, dg, at + 1:at + 2, :]], axis=1)
            return own, jnp.where(lane1 < 64, a_ref[2, dg, at:at + 1, :], a_ref[0, dg, at + 1:at + 2, :])

        value, variance, cell = rows_of(0), rows_of(1), rows_of(2)
        found = []
        for k, (lane, shift) in enumerate(((lane2, 0), (lane1, jnp.where(lane1 < 64, 0, 64)))):
            c = cell[k].astype(jnp.int32)
            target = (c >> 3) * 128 + ((lane >> 4) << 3) + (c & 7) + shift
            hot = jnp.where(iota((512, lane.shape[1]), 0) == target, 1.0, 0.0).astype(F32)
            high, low = split(pt[p, :, 512 * k:512 * k + 512])
            both_parts = mxu(jnp.concatenate([high, low], axis=0), hot)
            found.append(both_parts[0:48] + both_parts[48:96])
        whole = jnp.concatenate(found, axis=1)
        values = jnp.concatenate(value, axis=1)
        tail = whole[40:48]
        tail = jnp.where(iota((8, 384), 0) == 0, values - tail, 0.0)
        slab[p, 0:40, :] = whole[0:40]
        slab[p, 40:48, :] = tail
        inside = jnp.concatenate([jnp.ones((1, 256), F32), beside], axis=1) * in_grid[dg]
        inverse_of.append(inside / jnp.concatenate(variance, axis=1))

    third = lax.rem(iota((1, 384), 1) >> 4, 3)
    for a in range(2):
        for r in range(3):
            near = []
            for c in range(3):
                code = 3 * r + c
                taper = 1.0 if code == 4 else 0.5 if (r == 1 or c == 1) else 0.25
                chosen = jnp.zeros((1, 256), F32)
                for s in range(5):
                    blocks = ob_ref[5 * a + s:5 * a + s + 1, :]
                    chosen = chosen + jnp.where(blocks == code, taper, 0.0)
                chosen = jnp.concatenate([chosen, jnp.zeros((1, 128), F32)], axis=1)
                near.append(pltpu.roll(chosen, (16 * (c - 1)) % 384, 1) if c != 1 else chosen)
            for i in range(3):
                which = lax.rem(third + 4 - i, 3)
                w = jnp.where(which == 0, near[0], jnp.where(which == 1, near[1], near[2]))
                wc[a, 3 * r + i:3 * r + i + 1, :] = w * inverse_of[a + r]

    slot = lane1 >> 4
    block = block_of(lane1)
    own_slot = [(slot >= i) & (slot <= i + 2) for i in range(3)]
    diagonal = (lane1 - 40 * block == iota((40, 128), 0)) & (lane1 < 120)
    for g in range(6):
        turn = (16 - 48 * g) % 384

        def window(x):
            return (pltpu.roll(x, turn, 1) if turn else x)[:, 0:128]

        parts = [window(slab[p]) for p in range(4)]
        for a in range(2):
            weights = window(wc[a])
            left = jnp.concatenate(parts[a:a + 3], axis=1)
            right = []
            for i in range(3):
                right.append(jnp.concatenate([
                    parts[a + r][0:40] * jnp.where(own_slot[i], weights[3 * r + i:3 * r + i + 1], 0.0)
                    for r in range(3)], axis=1))
            right.append(jnp.zeros((8, 384), F32))
            right = jnp.concatenate(right, axis=0)
            lh, ll = split(left)
            rh, rl = split(right)
            o = mxu_nt(jnp.concatenate([lh, ll], axis=0), jnp.concatenate([rh, rl], axis=0))
            o = o[0:48] + o[48:96]
            o = o[:, 0:128] + o[:, 128:256]
            system = jnp.where(diagonal, 1.0, 0.0) + o[0:40] / (MEMBERS - 1.0)
            n = a * 6 + g
            gram[n, 0:40, :] = system
            gram[n, 40:48, :] = o[40:48] / (MEMBERS - 1.0)
            tr[n:n + 1, :] = jnp.sum(jnp.where(diagonal, system, 0.0), axis=0, keepdims=True)

    rows = tr[...]
    sums = [jnp.sum(jnp.where(block == i, rows, 0.0), axis=1, keepdims=True) for i in range(3)]
    tv[...] = jnp.where(block == 0, sums[0], jnp.where(block == 1, sums[1], sums[2]))
    for n in range(12):
        ps[n] = gram[n, 0:40, :] / tv[n:n + 1, :]
        zs[n] = jnp.where(diagonal, 1.0, 0.0)

    wide = jnp.concatenate([block, block], axis=1)

    def sweep(step, carry):
        for n in range(12):
            p, z = ps[n], zs[n]
            pair = jnp.concatenate(split(p), axis=1)
            stacked = three_high(pair, wide)
            right = jnp.concatenate([stacked, stacked], axis=0)
            o = mxu(jnp.concatenate([pair, jnp.concatenate(split(z), axis=1)], axis=0), right)
            o = o[:, 0:128] + o[:, 128:256]
            zs[n] = 1.5 * z - 0.5 * o[40:80]
            q = 1.5 * p - 0.5 * o[0:40]
            o = mxu(jnp.concatenate(split(q), axis=1), right)
            ps[n] = 1.5 * q - 0.5 * (o[:, 0:128] + o[:, 128:256])
        return carry

    lax.fori_loop(0, NS_ITERS - 1, sweep, 0)

    ones = jnp.where((block_of(iota((128, 128), 0)) == block) & (lane1 < 120), 1.0, 0.0).astype(F32)
    ones = jnp.concatenate([ones, ones], axis=0)
    patch = lax.rem(iota((1, 512), 1), 128) >> 3
    for a in range(2):
        total = jnp.zeros((40, 512), F32)
        ph, plow = split(pt[a + 1, 0:40, 0:512])
        for g in range(6):
            n = a * 6 + g
            p, z = ps[n], zs[n]
            pair = jnp.concatenate(split(p), axis=1)
            stacked = three_high(pair, wide)
            o = mxu(jnp.concatenate(split(z), axis=1), jnp.concatenate([stacked, stacked], axis=0))
            z = 1.5 * z - 0.5 * (o[:, 0:128] + o[:, 128:256])
            spread = z / jnp.sqrt(tv[n:n + 1, :])
            partial = mxu(jnp.concatenate(split(spread * gram[n, 40:41, :]), axis=1), ones)
            centre = jnp.sum(spread * partial, axis=0, keepdims=True)
            th, tl = split(spread + centre)
            high = three_high_by(ph, patch, 3 * g)
            low = three_high_by(plow, patch, 3 * g)
            total = total + mxu(jnp.concatenate([th, tl, th], axis=1), jnp.concatenate([high, high, low], axis=0))
        total = total + mean[a + 1]
        flat = out_ref.reshape(MEMBERS * 8, 128)
        for r in range(4):
            value = total[:, 128 * r:128 * r + 128]
            for s in range(LEVELS):
                flat[pl.ds(80 * s + 4 * a + r, 8, stride=8), :] = value[8 * s:8 * s + 8]
                flat[pl.ds(80 * s + 64 + 4 * a + r, 2, stride=8), :] = value[32 + 2 * s:34 + 2 * s]


def three_high_by(value, patch, first):
    parts = [jnp.where(patch == first + i, value, 0.0) for i in range(3)]
    return jnp.concatenate(parts + [jnp.zeros((8, value.shape[1]), F32)], axis=0)


def scratch_of():
    return [
        pltpu.VMEM((20, 40, 256), F32), pltpu.VMEM((20, 40, 256), F32),
        pltpu.VMEM((20, 1, 256), F32), pltpu.VMEM((20, 1, 256), F32),
        pltpu.VMEM((4, 48, 1024), F32), pltpu.VMEM((4, 1, 512), F32),
        pltpu.VMEM((4, 48, 384), F32), pltpu.VMEM((2, 9, 384), F32),
        pltpu.VMEM((12, 48, 128), F32), pltpu.VMEM((12, 128), F32), pltpu.VMEM((12, 128), F32),
        pltpu.VMEM((12, 40, 128), F32), pltpu.VMEM((12, 40, 128), F32)]


def solution(mesh):
    n_gx, n_gy = mesh.shape["gx"], mesh.shape["gy"]
    dma = pltpu.SemaphoreType.DMA

    def local(*args):
        def body(*refs):
            cycle_kernel(n_gx, n_gy, *refs)

        return pl.pallas_call(
            body, out_shape=jax.ShapeDtypeStruct((OWN, LEVELS, 8, 128), F32),
            in_specs=[pl.BlockSpec(memory_space=pl.ANY)] * 7, out_specs=pl.BlockSpec(memory_space=pltpu.VMEM),
            scratch_shapes=[pltpu.VMEM(a.shape, a.dtype) for a in args] + [
                pltpu.VMEM((LEVELS, 80, 128), F32), pltpu.VMEM((AUX, 128), F32), pltpu.VMEM((16, 256), F32),
                pltpu.VMEM((3, 3, LEVELS, 80, 128), F32), pltpu.VMEM((3, 3, AUX, 128), F32),
                pltpu.VMEM((LEVELS, OWN, 8, 128), F32)] + scratch_of() + [
                dma((3, LEVELS)), dma((3, LEVELS)), dma((3,)), dma((3,)),
                dma((2, 3, LEVELS + 1)), dma((2, 3, LEVELS + 1)), dma((7,)), dma((LEVELS,)), dma((LEVELS,))],
            compiler_params=pltpu.CompilerParams(collective_id=0, has_side_effects=True),
            name="cycle")(*args)

    return jax.shard_map(
        local,
        mesh=mesh,
        in_specs=(
            P("mem", None, "gx", "gy"),
            P(None, "gx", "gy"),
            P("gx", "gy"),
            P(None, None, "gx", "gy"),
            P(None, None, "gx", "gy"),
            P(None, None, "gx", "gy"),
            P(None, "gx", "gy"),
        ),
        out_specs=P("mem", None, "gx", "gy"),
        check_vma=False,
    )
```

```python
import jax
import jax.numpy as jnp
from jax import lax
from jax.experimental import pallas as pl
from jax.experimental.pallas import tpu as pltpu
from jax.sharding import PartitionSpec as P

MESH = pl.DeviceIdType.MESH
F32 = jnp.float32
NS_ITERS = 7
BY_ROWS = (False, False, False)
LEVELS = 4
OWN = 10
MEMBERS = 40
OBS = 16
AUX = 32
NEED = ((16, 64), (0, 80), (0, 64))


def neighbours(n_gx, n_gy):
    mem, gx, gy = lax.axis_index("mem"), lax.axis_index("gx"), lax.axis_index("gy")
    rows = (lax.rem(gx + n_gx - 1, n_gx), gx, lax.rem(gx + 1, n_gx))
    sides = (lax.rem(gy + n_gy - 1, n_gy), lax.rem(gy + 1, n_gy))
    there = [lax.rem(mem + o, LEVELS) for o in range(LEVELS)]
    back = [lax.rem(mem + LEVELS - o, LEVELS) for o in range(LEVELS)]
    return mem, gx, gy, rows, sides, there, back


def prepare(level, x_ref, dif_ref, mask_ref, val_ref, var_ref, cell_ref, blk_ref, xs, aux, ob):
    flat = x_ref.reshape(OWN * LEVELS * 8, 128)
    for k in range(LEVELS):
        for r in range(8):
            main = 8 * r if r < 2 else 16 + 8 * r
            xs[k, main:main + 8, :] = flat[pl.ds(k * 8 + r, 8, stride=32), :]
            xs[k, 16 + 2 * r:18 + 2 * r, :] = flat[pl.ds(256 + k * 8 + r, 2, stride=32), :]
    aux[0:8, :] = dif_ref[level]
    aux[8:16, :] = mask_ref[...].astype(F32)
    spread_out = jnp.where(iota((16, 256), 0) == iota((16, 256), 1) >> 4, 1.0, 0.0).astype(F32)
    kinds = [ref[level].astype(F32) for ref in (val_ref, var_ref, cell_ref)]
    stacked = jnp.concatenate([kinds[k][:, a, :] for a in range(2) for k in range(3)], axis=0)
    wide = lax.dot_general(stacked, spread_out, (((1,), (0,)), ((), ())), precision=lax.Precision.HIGHEST,
                           preferred_element_type=F32)
    mine = iota((16, 256), 0) == (iota((16, 256), 1) & 15)
    for n in range(6):
        row = jnp.sum(jnp.where(mine, wide[16 * n:16 * n + 16], 0.0), axis=0, keepdims=True)
        aux[16 + 2 * n:17 + 2 * n, :] = row[:, 0:128]
        aux[17 + 2 * n:18 + 2 * n, :] = row[:, 128:256]
    aux[28:32, :] = jnp.zeros((4, 128), F32)
    blocks = blk_ref[...].astype(F32)
    blocks = jnp.concatenate([blocks[:, a, :] for a in range(2)] + [jnp.zeros((6, 16), F32)], axis=0)
    ob[...] = mxu(blocks, spread_out)


def cycle_kernel(n_gx, n_gy, x_any, dif_any, mask_any, val_any, var_any, cell_any, blk_any, out_ref,
                 x_ref, dif_ref, mask_ref, val_ref, var_ref, cell_ref, blk_ref, xs, aux, ob, g_ref, a_ref, y_ref, *rest):
    scratch, (ssem, rsem, asem, arsem, fsem, frsem, lsem, bsem, brsem) = rest[:-9], rest[-9:]
    mem, gx, gy, rows, sides, there, back = neighbours(n_gx, n_gy)

    in_rows = (gx > 0, None, gx < n_gx - 1)
    in_sides = (gy > 0, gy < n_gy - 1)

    def when(*conditions):
        known = [c for c in conditions if c is not None]
        if not known:
            return lambda f: f()
        return pl.when(known[0] if len(known) == 1 else known[0] & known[1])

    barrier = pltpu.get_barrier_semaphore()
    count = LEVELS - 1
    for d in range(3):
        @when(in_rows[d])
        def _():
            for o in range(1, LEVELS) if d == 1 else (0,):
                pl.semaphore_signal(barrier, inc=1, device_id=(there[o], rows[d], gy), device_id_type=MESH)
        if d != 1:
            count = count + jnp.where(in_rows[d], 1, 0)
    for e in range(2):
        @when(in_sides[e])
        def _():
            pl.semaphore_signal(barrier, inc=1, device_id=(mem, gx, sides[e]), device_id_type=MESH)
        count = count + jnp.where(in_sides[e], 1, 0)

    loads = [pltpu.make_async_copy(src, dst, lsem.at[n]) for n, (src, dst) in enumerate((
        (x_any, x_ref), (dif_any, dif_ref), (mask_any, mask_ref), (val_any, val_ref), (var_any, var_ref),
        (cell_any, cell_ref), (blk_any, blk_ref)))]
    for load in loads:
        load.start()
    for load in loads:
        load.wait()
    prepare(mem, x_ref, dif_ref, mask_ref, val_ref, var_ref, cell_ref, blk_ref, xs, aux, ob)
    f0, f1, dif, wet, pt, hot, obs, slab, wc = scratch[:9]
    grid = masks(n_gx, n_gy)
    for dg in (0, 2):
        @when(~in_rows[dg])
        def _():
            for h in range(3):
                g_ref[h, dg] = jnp.zeros((LEVELS, 80, 128), F32)
                a_ref[h, dg] = jnp.ones((AUX, 128), F32)
    for h in (0, 2):
        @when(~in_sides[h // 2])
        def _():
            g_ref[h] = jnp.zeros((3, LEVELS, 80, 128), F32)
            a_ref[h] = jnp.ones((3, AUX, 128), F32)
    pl.semaphore_wait(barrier, count)

    sends = []

    def start(copy, *conditions):
        when(*conditions)(copy.start)
        sends.append((copy, conditions))

    def forward(source, dg, slot, part, index):
        for e, side in enumerate(sides):
            h = 2 if e == 0 else 0
            dst = a_ref.at[h, dg] if slot is None else g_ref.at[h, dg, slot, part]
            start(pltpu.make_async_remote_copy(
                src_ref=source, dst_ref=dst, send_sem=fsem.at[e, dg, index], recv_sem=frsem.at[h // 2, dg, index],
                device_id=(mem, gx, side), device_id_type=MESH), in_rows[dg], in_sides[e])

    def scatter(o):
        start(pltpu.make_async_remote_copy(
            src_ref=xs.at[there[o]], dst_ref=g_ref.at[1, 1, mem], send_sem=ssem.at[1, o], recv_sem=rsem.at[1, o],
            device_id=(there[o], gx, gy), device_id_type=MESH))

    def halo(source, slot, o):
        for d in (0, 2):
            part = pl.ds(*NEED[2 - d])
            start(pltpu.make_async_remote_copy(
                src_ref=source.at[part], dst_ref=g_ref.at[1, 2 - d, slot, part],
                send_sem=ssem.at[d, o], recv_sem=rsem.at[2 - d, o],
                device_id=(mem, rows[d], gy), device_id_type=MESH), in_rows[d])

    def scatter_aux(d):
        start(pltpu.make_async_remote_copy(
            src_ref=aux, dst_ref=a_ref.at[1, 2 - d], send_sem=asem.at[d], recv_sem=arsem.at[2 - d],
            device_id=(mem, rows[d], gy), device_id_type=MESH), in_rows[d])

    forward(aux, 1, None, None, LEVELS)
    forward(xs.at[mem], 1, mem, pl.ds(0, 80), 0)
    for o in range(1, LEVELS):
        scatter(o)
    halo(xs.at[mem], mem, 0)
    for d in (0, 2):
        scatter_aux(d)
    g_ref[1, 1, mem] = xs[mem]
    a_ref[1, 1] = aux[...]

    def arrival(dg, o):
        part = pl.ds(*NEED[dg])

        @when(in_rows[dg])
        def _():
            pltpu.make_async_remote_copy(
                src_ref=xs.at[0, part], dst_ref=g_ref.at[1, dg, back[o], part],
                send_sem=ssem.at[dg, o], recv_sem=rsem.at[dg, o],
                device_id=(mem, rows[dg], gy), device_id_type=MESH).wait_recv()
        if dg == 1:
            halo(g_ref.at[1, 1, back[o]], back[o], o)
        forward(g_ref.at[1, dg, back[o], part], dg, back[o], part, o)

    for o in (1, 3, 2):
        arrival(1, o)
    for dg in (0, 2):
        @when(in_rows[dg])
        def _():
            pltpu.make_async_remote_copy(
                src_ref=aux, dst_ref=a_ref.at[1, dg], send_sem=asem.at[dg], recv_sem=arsem.at[dg],
                device_id=(mem, rows[dg], gy), device_id_type=MESH).wait_recv()
        forward(a_ref.at[1, dg], dg, None, None, LEVELS)
    def passed_on(h, dg, chunks):
        @when(in_sides[h // 2], in_rows[dg])
        def _():
            for o in range(LEVELS) if chunks else ():
                part = pl.ds(*NEED[dg])
                pltpu.make_async_remote_copy(
                    src_ref=xs.at[0, part], dst_ref=g_ref.at[h, dg, back[o], part],
                    send_sem=fsem.at[0, dg, o], recv_sem=frsem.at[h // 2, dg, o],
                    device_id=(mem, gx, sides[0]), device_id_type=MESH).wait_recv()
            if not chunks:
                pltpu.make_async_remote_copy(
                    src_ref=aux, dst_ref=a_ref.at[h, dg],
                    send_sem=fsem.at[0, dg, LEVELS], recv_sem=frsem.at[h // 2, dg, LEVELS],
                    device_id=(mem, gx, sides[0]), device_id_type=MESH).wait_recv()

    weigh(ob, wc)
    for dg in (0, 2):
        arrival(dg, 0)
    for h in (0, 2):
        passed_on(h, 1, True)
        for dg in (1, 0, 2):
            passed_on(h, dg, False)
    assemble(grid, g_ref, a_ref, f0, dif, wet, (1,))
    forecast(f0, f1, dif, wet, pt, ((7, 10), 3), ((8, 10), 2))
    aim(grid, a_ref, hot, obs, wc)
    for o in (1, 3, 2):
        for dg in (0, 2):
            arrival(dg, o)
    for h in (0, 2):
        for dg in (0, 2):
            passed_on(h, dg, True)
    assemble(grid, g_ref, a_ref, f0, dif, wet, (0, 2))
    forecast(f0, f1, dif, wet, pt, ((1, 13), 6), ((2, 12), 6))
    analyse(grid, y_ref, pt, hot, obs, slab, wc, *scratch[9:])

    for o in range(1, LEVELS):
        start(pltpu.make_async_remote_copy(
            src_ref=y_ref.at[there[o]], dst_ref=out_ref.at[:, mem], send_sem=bsem.at[o], recv_sem=brsem.at[o],
            device_id=(there[o], gx, gy), device_id_type=MESH))
    out_ref[:, mem] = y_ref[mem]
    for o in range(1, LEVELS):
        pltpu.make_async_remote_copy(
            src_ref=y_ref.at[0], dst_ref=out_ref.at[:, back[o]], send_sem=bsem.at[o], recv_sem=brsem.at[o],
            device_id=(there[o], gx, gy), device_id_type=MESH).wait_recv()
    for copy, conditions in sends:
        when(*conditions)(copy.wait_send)


def split(x):
    high = x.astype(jnp.bfloat16).astype(F32)
    return high, x - high


def mxu(a, b):
    return lax.dot_general(a, b, (((1,), (0,)), ((), ())), preferred_element_type=F32)


def mxu_nt(a, b):
    return lax.dot_general(a, b, (((1,), (1,)), ((), ())), preferred_element_type=F32)


def iota(shape, axis):
    return lax.broadcasted_iota(jnp.int32, shape, axis)


def block_of(lane):
    return jnp.where(lane < 40, 0, jnp.where(lane < 80, 1, jnp.where(lane < 120, 2, 3)))


def three_high(value, block):
    parts = [jnp.where(block == i, value, 0.0) for i in range(3)]
    return jnp.concatenate(parts + [jnp.zeros((8, value.shape[1]), F32)], axis=0)


def masks(n_gx, n_gy):
    gx, gy = lax.axis_index("gx"), lax.axis_index("gy")
    one = lambda c: jnp.where(c, 1.0, 0.0).astype(F32)
    lane1 = iota((1, 128), 1)
    in_grid = (one(gx > 0), jnp.float32(1.0), one(gx < n_gx - 1))
    return in_grid, jnp.where(lane1 < 64, one(gy < n_gy - 1), one(gy > 0)), lane1


def weigh(ob_ref, wc):
    third = lax.rem(iota((1, 384), 1) >> 4, 3)
    for a in range(2):
        for r in range(3):
            near = []
            for c in range(3):
                code = 3 * r + c
                taper = 1.0 if code == 4 else 0.5 if (r == 1 or c == 1) else 0.25
                chosen = jnp.zeros((1, 256), F32)
                for s in range(5):
                    blocks = ob_ref[5 * a + s:5 * a + s + 1, :]
                    chosen = chosen + jnp.where(blocks == code, taper, 0.0)
                chosen = jnp.concatenate([chosen, jnp.zeros((1, 128), F32)], axis=1)
                near.append(pltpu.roll(chosen, (16 * (c - 1)) % 384, 1) if c != 1 else chosen)
            for i in range(3):
                which = lax.rem(third + 4 - i, 3)
                wc[a, 3 * r + i:3 * r + i + 1, :] = jnp.where(
                    which == 0, near[0], jnp.where(which == 1, near[1], near[2]))


def assemble(grid, g_ref, a_ref, f0, dif, wet, groups):
    in_grid, beside, lane1 = grid

    def both(h_of, dg):
        own, side = h_of(1), jnp.where(lane1 < 64, h_of(2), h_of(0)) * (beside * in_grid[dg])
        return (own if dg == 1 else own * in_grid[dg]), side

    for t in range(20):
        dg, r = (0, t + 2) if t < 6 else (1, t - 6) if t < 14 else (2, t - 14)
        if dg not in groups:
            continue
        main = 8 * r if r < 2 else 16 + 8 * r
        rest = 16 + 2 * r
        for s in range(LEVELS):
            own, side = both(lambda h: g_ref[h, dg, s, main:main + 8, :], dg)
            f0[t, 8 * s:8 * s + 8, 0:128] = own
            f0[t, 8 * s:8 * s + 8, 128:256] = side
            own, side = both(lambda h: g_ref[h, dg, s, rest:rest + 2, :], dg)
            f0[t, 32 + 2 * s:34 + 2 * s, 0:128] = own
            f0[t, 32 + 2 * s:34 + 2 * s, 128:256] = side
        own, side = both(lambda h: a_ref[h, dg, r:r + 1, :], dg)
        dif[t, :, 0:128] = own
        dif[t, :, 128:256] = side
        own, side = both(lambda h: a_ref[h, dg, 8 + r:9 + r, :], dg)
        wet[t, :, 0:128] = own
        wet[t, :, 128:256] = side


def advance(src, dif, wet, t):
    c = src[t]
    around = src[t + 1] + src[t - 1]
    around = around + pltpu.roll(c, 255, 1) + pltpu.roll(c, 1, 1)
    return wet[t] * (c + dif[t] * (around - 4.0 * c))


def forecast(f0, f1, dif, wet, pt, first, second):
    def one(k, carry):
        for low in first[0]:
            f1[low + k] = advance(f0, dif, wet, low + k)
        return carry

    lax.fori_loop(0, first[1], one, 0)

    def two(k, carry):
        for low in second[0]:
            value = advance(f1, dif, wet, low + k)
            m = jnp.sum(value, axis=0, keepdims=True) / MEMBERS
            pt[low + k - 2, 0:40, :] = value - m
            pt[low + k - 2, 40:48, :] = jnp.where(iota((8, 256), 0) == 0, m, 0.0)
        return carry

    lax.fori_loop(0, second[1], two, 0)


def aim(grid, a_ref, hot, obs, wc):
    in_grid, beside, lane1 = grid
    lane2 = iota((1, 256), 1)
    for p in range(4):
        dg, a = ((0, 1), (1, 0), (1, 1), (2, 0))[p]

        def rows_of(kind):
            at = 16 + (a * 3 + kind) * 2
            own = jnp.concatenate([a_ref[1, dg, at:at + 1, :], a_ref[1, dg, at + 1:at + 2, :]], axis=1)
            return own, jnp.where(lane1 < 64, a_ref[2, dg, at:at + 1, :], a_ref[0, dg, at + 1:at + 2, :])

        value, variance, cell = rows_of(0), rows_of(1), rows_of(2)
        for k, (lane, shift) in enumerate(((lane2, 0), (lane1, jnp.where(lane1 < 64, 0, 64)))):
            c = cell[k].astype(jnp.int32)
            target = (c >> 3) * 128 + ((lane >> 4) << 3) + (c & 7) + shift
            at, width = 256 * k, lane.shape[1]

            def fill(n, carry):
                top = pl.multiple_of(n * 64, 64)
                hot[p, pl.ds(top, 64), at:at + width] = jnp.where(
                    iota((64, width), 0) == target - n * 64, 1.0, 0.0).astype(F32)
                return carry

            lax.fori_loop(0, 8, fill, 0)
        obs[p:p + 1, :] = jnp.concatenate(value, axis=1)
        inside = jnp.concatenate([jnp.ones((1, 256), F32), beside], axis=1) * in_grid[dg]
        obs[4 + p:5 + p, :] = inside / jnp.concatenate(variance, axis=1)
    for a in range(2):
        for r in range(3):
            p = a + r
            rows = wc[a, 3 * r:3 * r + 3, :] * obs[4 + p:5 + p, :]
            wc[a, 3 * r:3 * r + 3, :] = pltpu.roll(rows, 80 * (p % 3), 1) if p % 3 else rows


GROUPS = 11


def analyse(grid, y_ref, pt, hot, obs, slab, wc, gram, tr, tv, ps, zs):
    lane1 = grid[2]

    for p in range(4):
        found = []
        for k, (low, high) in enumerate(((0, 256), (256, 384))):
            rows = jnp.concatenate([pt[4 * p + r, :, 128 * k:128 * k + 128] for r in range(4)], axis=1)
            both_parts = mxu(jnp.concatenate(split(rows), axis=0), hot[p, :, low:high])
            found.append(both_parts[0:48] + both_parts[48:96])
        whole = jnp.concatenate(found, axis=1)
        tail = jnp.where(iota((8, 384), 0) == 0, obs[p:p + 1, :] - whole[40:48], 0.0)
        whole = jnp.concatenate([whole[0:40], tail], axis=0)
        slab[p] = pltpu.roll(whole, 80 * (p % 3), 1) if p % 3 else whole

    lane2 = iota((1, 256), 1)
    part = jnp.where(lane2 < 80, 0, jnp.where(lane2 < 160, 1, jnp.where(lane2 < 240, 2, 3)))
    slot = (lane2 - 80 * part) >> 4
    block = block_of(lane1)
    diagonal = (lane1 - 40 * block == iota((40, 128), 0)) & (lane1 < 120)

    def keep(n, o):
        system = jnp.where(diagonal, 1.0, 0.0) + o[0:40] / (MEMBERS - 1.0)
        gram[n, 0:40, :] = system
        gram[n, 40:48, :] = o[40:48] / (MEMBERS - 1.0)
        tr[n:n + 1, :] = jnp.sum(jnp.where(diagonal, system, 0.0), axis=0, keepdims=True)

    last = []
    for g in range(6):
        turn = (16 - 48 * g) % 384

        def window(x):
            return pltpu.roll(x, turn, 1)[:, 0:256]

        parts = [window(slab[p]) for p in range(4)]
        for a in range(2):
            left = jnp.where(part == 0, parts[3 * a], jnp.where(part == 1, parts[1], parts[2]))
            weights = window(wc[a])
            right = []
            for i in range(3):
                w = jnp.zeros((1, 256), F32)
                for r in range(3):
                    w = jnp.where(part == (a + r) % 3, weights[3 * r + i:3 * r + i + 1], w)
                w = jnp.where((part < 3) & (slot >= i) & (slot <= i + 2), w, 0.0)
                right.append(left[0:40] * w)
            right.append(jnp.zeros((8, 256), F32))
            right = jnp.concatenate(right, axis=0)
            o = mxu_nt(jnp.concatenate(split(left), axis=0), jnp.concatenate(split(right), axis=0))
            o = o[0:48] + o[48:96]
            o = o[:, 0:128] + o[:, 128:256]
            if g < 5:
                keep(2 * g + a, o)
            else:
                last.append(o)
    keep(10, jnp.where(block == 0, last[0], jnp.where(block == 1, pltpu.roll(last[1], 40, 1), 0.0)))
    tr[11:12, :] = jnp.ones((1, 128), F32)

    rows = tr[...]
    sums = [jnp.sum(jnp.where(block == i, rows, 0.0), axis=1, keepdims=True) for i in range(3)]
    tv[...] = jnp.where(block == 0, sums[0], jnp.where(block == 1, sums[1], sums[2]))
    for n in range(GROUPS):
        ps[n] = gram[n, 0:40, :] / tv[n:n + 1, :]
        zs[n] = jnp.where(diagonal, 1.0, 0.0)

    wide = jnp.concatenate([block, block], axis=1)

    def times(rows_of, stacked, by_rows):
        count = len(rows_of)
        if by_rows:
            o = mxu(jnp.concatenate([x for v in rows_of for x in split(v)], axis=0), stacked)
            o = [o[80 * k:80 * k + 40] + o[80 * k + 40:80 * k + 80] for k in range(count)]
        else:
            o = mxu(jnp.concatenate([jnp.concatenate(split(v), axis=1) for v in rows_of], axis=0),
                    jnp.concatenate([stacked, stacked], axis=0))
            o = [o[40 * k:40 * k + 40] for k in range(count)]
        return [x[:, 0:128] + x[:, 128:256] for x in o]

    def sweep(step, carry):
        for n in range(GROUPS):
            p, z = ps[n], zs[n]
            stacked = three_high(jnp.concatenate(split(p), axis=1), wide)
            pp, zp = times([p, z], stacked, BY_ROWS[0])
            zs[n] = 1.5 * z - 0.5 * zp
            q = 1.5 * p - 0.5 * pp
            ps[n] = 1.5 * q - 0.5 * times([q], stacked, BY_ROWS[1])[0]
        return carry

    lax.fori_loop(0, NS_ITERS - 1, sweep, 0)

    ones = jnp.where((block_of(iota((128, 128), 0)) == block) & (lane1 < 120), 1.0, 0.0).astype(F32)
    spreads, columns = [], []
    for n in range(GROUPS):
        z = zs[n]
        stacked = three_high(jnp.concatenate(split(ps[n]), axis=1), wide)
        z = 1.5 * z - 0.5 * times([z], stacked, BY_ROWS[2])[0]
        spreads.append(z / jnp.sqrt(tv[n:n + 1, :]))
        columns.append(jnp.concatenate(split(spreads[n] * gram[n, 40:41, :]), axis=1))
    partial = mxu(jnp.concatenate(columns, axis=0), jnp.concatenate([ones, ones], axis=0))
    transforms = []
    for n in range(GROUPS):
        centre = jnp.sum(spreads[n] * partial[40 * n:40 * n + 40], axis=0, keepdims=True)
        th, tl = split(spreads[n] + centre)
        transforms.append(jnp.concatenate([
            jnp.concatenate([th, th], axis=1), jnp.concatenate([tl, jnp.zeros_like(tl)], axis=1)], axis=0))

    patch = lax.rem(iota((1, 512), 1), 128) >> 3
    flat = y_ref.reshape(MEMBERS * 8, 128)
    for a in range(2):
        here = jnp.concatenate([pt[4 + 4 * a + r, 0:40, 0:128] for r in range(4)], axis=1)
        here = split(here)
        total = jnp.zeros((80, 512), F32)
        for g in range(6):
            n = 2 * g + a if g < 5 else 10
            ids = (3 * g, 3 * g + 1, 3 * g + 2) if g < 5 else (15, -1, -1) if a == 0 else (-1, 15, -1)
            pieces = []
            for v in here:
                pieces += [jnp.where(patch == c, v, 0.0) if c >= 0 else jnp.zeros((40, 512), F32) for c in ids]
                pieces.append(jnp.zeros((8, 512), F32))
            total = total + mxu(transforms[n], jnp.concatenate(pieces, axis=0))
        total = total[0:40] + total[40:80]
        for r in range(4):
            value = total[:, 128 * r:128 * r + 128] + pt[4 + 4 * a + r, 40:41, 0:128]
            for s in range(LEVELS):
                flat[pl.ds(80 * s + 4 * a + r, 8, stride=8), :] = value[8 * s:8 * s + 8]
                flat[pl.ds(80 * s + 64 + 4 * a + r, 2, stride=8), :] = value[32 + 2 * s:34 + 2 * s]


def compute_kernel(n_gx, n_gy, g_ref, a_ref, ob, y_ref, f0, f1, dif, wet, pt, hot, obs, slab, wc, *rest):
    grid = masks(n_gx, n_gy)
    weigh(ob, wc)
    aim(grid, a_ref, hot, obs, wc)
    assemble(grid, g_ref, a_ref, f0, dif, wet, (1,))
    forecast(f0, f1, dif, wet, pt, ((7, 10), 3), ((8, 10), 2))
    assemble(grid, g_ref, a_ref, f0, dif, wet, (0, 2))
    forecast(f0, f1, dif, wet, pt, ((1, 13), 6), ((2, 12), 6))
    analyse(grid, y_ref, pt, hot, obs, slab, wc, *rest)


def scratch_of():
    return [
        pltpu.VMEM((20, 40, 256), F32), pltpu.VMEM((20, 40, 256), F32),
        pltpu.VMEM((20, 1, 256), F32), pltpu.VMEM((20, 1, 256), F32),
        pltpu.VMEM((16, 48, 256), F32), pltpu.VMEM((4, 512, 384), F32), pltpu.VMEM((8, 384), F32),
        pltpu.VMEM((4, 48, 384), F32), pltpu.VMEM((2, 16, 384), F32),
        pltpu.VMEM((12, 48, 128), F32), pltpu.VMEM((12, 128), F32), pltpu.VMEM((12, 128), F32),
        pltpu.VMEM((12, 40, 128), F32), pltpu.VMEM((12, 40, 128), F32)]


def solution(mesh):
    n_gx, n_gy = mesh.shape["gx"], mesh.shape["gy"]
    dma = pltpu.SemaphoreType.DMA

    def local(*args):
        def body(*refs):
            cycle_kernel(n_gx, n_gy, *refs)

        return pl.pallas_call(
            body, out_shape=jax.ShapeDtypeStruct((OWN, LEVELS, 8, 128), F32),
            in_specs=[pl.BlockSpec(memory_space=pl.ANY)] * 7, out_specs=pl.BlockSpec(memory_space=pltpu.VMEM),
            scratch_shapes=[pltpu.VMEM(a.shape, a.dtype) for a in args] + [
                pltpu.VMEM((LEVELS, 80, 128), F32), pltpu.VMEM((AUX, 128), F32), pltpu.VMEM((16, 256), F32),
                pltpu.VMEM((3, 3, LEVELS, 80, 128), F32), pltpu.VMEM((3, 3, AUX, 128), F32),
                pltpu.VMEM((LEVELS, OWN, 8, 128), F32)] + scratch_of() + [
                dma((3, LEVELS)), dma((3, LEVELS)), dma((3,)), dma((3,)),
                dma((2, 3, LEVELS + 1)), dma((2, 3, LEVELS + 1)), dma((7,)), dma((LEVELS,)), dma((LEVELS,))],
            compiler_params=pltpu.CompilerParams(collective_id=0, has_side_effects=True),
            name="cycle")(*args)

    return jax.shard_map(
        local,
        mesh=mesh,
        in_specs=(
            P("mem", None, "gx", "gy"),
            P(None, "gx", "gy"),
            P("gx", "gy"),
            P(None, None, "gx", "gy"),
            P(None, None, "gx", "gy"),
            P(None, None, "gx", "gy"),
            P(None, "gx", "gy"),
        ),
        out_specs=P("mem", None, "gx", "gy"),
        check_vma=False,
    )
```

```python
import jax
import jax.numpy as jnp
from jax import lax
from jax.experimental import pallas as pl
from jax.experimental.pallas import tpu as pltpu
from jax.sharding import PartitionSpec as P

MESH = pl.DeviceIdType.MESH
F32 = jnp.float32
NS_ITERS = 7
BY_ROWS = (False, False, False)
LEVELS = 4
OWN = 10
MEMBERS = 40
OBS = 16
MAIN = (64, 72, 20, 28, 36, 44, 0, 8)
REST = (60, 62, 52, 54, 56, 58, 16, 18)
AUX = 28
FLOW = (6, 7, 10, 11, 12, 13, 18, 19)
WET = (8, 9, 14, 15, 16, 17, 20, 21)
SEEN = (0, 22)
NEED = ((0, 60), (0, 80), (20, 60))
NEED_AUX = ((10, 18), (0, 28), (0, 18))


def neighbours(n_gx, n_gy):
    mem, gx, gy = lax.axis_index("mem"), lax.axis_index("gx"), lax.axis_index("gy")
    rows = (lax.rem(gx + n_gx - 1, n_gx), gx, lax.rem(gx + 1, n_gx))
    sides = (lax.rem(gy + n_gy - 1, n_gy), lax.rem(gy + 1, n_gy))
    there = [lax.rem(mem + o, LEVELS) for o in range(LEVELS)]
    back = [lax.rem(mem + LEVELS - o, LEVELS) for o in range(LEVELS)]
    return mem, gx, gy, rows, sides, there, back


def lay_out(x_ref, xs):
    flat = x_ref.reshape(OWN * LEVELS * 8, 128)
    for k in range(LEVELS):
        for r in range(8):
            xs[k, MAIN[r]:MAIN[r] + 8, :] = flat[pl.ds(k * 8 + r, 8, stride=32), :]
            xs[k, REST[r]:REST[r] + 2, :] = flat[pl.ds(256 + k * 8 + r, 2, stride=32), :]


def prepare(level, dif_ref, mask_ref, val_ref, var_ref, cell_ref, blk_ref, aux, ob):
    for rows, value in ((FLOW, dif_ref[level]), (WET, mask_ref[...].astype(F32))):
        for r in range(8):
            aux[rows[r]:rows[r] + 1, :] = value[r:r + 1]
    spread_out = jnp.where(iota((16, 256), 0) == iota((16, 256), 1) >> 4, 1.0, 0.0).astype(F32)
    kinds = [ref[level].astype(F32) for ref in (val_ref, var_ref, cell_ref)]
    stacked = jnp.concatenate([kinds[k][:, a, :] for a in range(2) for k in range(3)], axis=0)
    wide = lax.dot_general(stacked, spread_out, (((1,), (0,)), ((), ())), precision=lax.Precision.HIGHEST,
                           preferred_element_type=F32)
    mine = iota((16, 256), 0) == (iota((16, 256), 1) & 15)
    for n in range(6):
        row = jnp.sum(jnp.where(mine, wide[16 * n:16 * n + 16], 0.0), axis=0, keepdims=True)
        at = SEEN[n // 3] + 2 * (n % 3)
        aux[at:at + 1, :] = row[:, 0:128]
        aux[at + 1:at + 2, :] = row[:, 128:256]
    blocks = blk_ref[...].astype(F32)
    blocks = jnp.concatenate([blocks[:, a, :] for a in range(2)] + [jnp.zeros((6, 16), F32)], axis=0)
    ob[...] = mxu(blocks, spread_out)


def cycle_kernel(n_gx, n_gy, x_any, dif_any, mask_any, val_any, var_any, cell_any, blk_any, out_ref,
                 x_ref, dif_ref, mask_ref, val_ref, var_ref, cell_ref, blk_ref, xs, aux, ob, g_ref, a_ref, y_ref, *rest):
    scratch, (ssem, rsem, asem, arsem, fsem, frsem, lsem, bsem, brsem) = rest[:-9], rest[-9:]
    mem, gx, gy, rows, sides, there, back = neighbours(n_gx, n_gy)

    in_rows = (gx > 0, None, gx < n_gx - 1)
    in_sides = (gy > 0, gy < n_gy - 1)

    def when(*conditions):
        known = [c for c in conditions if c is not None]
        if not known:
            return lambda f: f()
        return pl.when(known[0] if len(known) == 1 else known[0] & known[1])

    barrier = pltpu.get_barrier_semaphore()
    count = LEVELS - 1
    for d in range(3):
        @when(in_rows[d])
        def _():
            for o in range(1, LEVELS) if d == 1 else (0,):
                pl.semaphore_signal(barrier, inc=1, device_id=(there[o], rows[d], gy), device_id_type=MESH)
        if d != 1:
            count = count + jnp.where(in_rows[d], 1, 0)
    for e in range(2):
        @when(in_sides[e])
        def _():
            pl.semaphore_signal(barrier, inc=1, device_id=(mem, gx, sides[e]), device_id_type=MESH)
        count = count + jnp.where(in_sides[e], 1, 0)

    loads = [pltpu.make_async_copy(src, dst, lsem.at[n]) for n, (src, dst) in enumerate((
        (x_any, x_ref), (dif_any, dif_ref), (mask_any, mask_ref), (val_any, val_ref), (var_any, var_ref),
        (cell_any, cell_ref), (blk_any, blk_ref)))]
    for load in loads:
        load.start()
    loads[0].wait()
    lay_out(x_ref, xs)
    f0, f1, dif, wet, pt, hot, obs, slab, wc = scratch[:9]
    grid = masks(n_gx, n_gy)
    pl.semaphore_wait(barrier, count)

    sends = []

    def start(copy, *conditions):
        when(*conditions)(copy.start)
        sends.append((copy, conditions))

    def forward(source, dg, slot, part, index):
        for e, side in enumerate(sides):
            h = 2 if e == 0 else 0
            dst = a_ref.at[h, dg, part] if slot is None else g_ref.at[h, dg, slot, part]
            start(pltpu.make_async_remote_copy(
                src_ref=source, dst_ref=dst, send_sem=fsem.at[e, dg, index], recv_sem=frsem.at[h // 2, dg, index],
                device_id=(mem, gx, side), device_id_type=MESH), in_rows[dg], in_sides[e])

    def scatter(o):
        start(pltpu.make_async_remote_copy(
            src_ref=xs.at[there[o]], dst_ref=g_ref.at[1, 1, mem], send_sem=ssem.at[1, o], recv_sem=rsem.at[1, o],
            device_id=(there[o], gx, gy), device_id_type=MESH))

    def halo(source, slot, o):
        for d in (0, 2):
            part = pl.ds(*NEED[2 - d])
            start(pltpu.make_async_remote_copy(
                src_ref=source.at[part], dst_ref=g_ref.at[1, 2 - d, slot, part],
                send_sem=ssem.at[d, o], recv_sem=rsem.at[2 - d, o],
                device_id=(mem, rows[d], gy), device_id_type=MESH), in_rows[d])

    def scatter_aux(d):
        part = pl.ds(*NEED_AUX[2 - d])
        start(pltpu.make_async_remote_copy(
            src_ref=aux.at[part], dst_ref=a_ref.at[1, 2 - d, part], send_sem=asem.at[d], recv_sem=arsem.at[2 - d],
            device_id=(mem, rows[d], gy), device_id_type=MESH), in_rows[d])

    for o in (2, 1, 3):
        scatter(o)
    halo(xs.at[mem], mem, 0)
    forward(xs.at[mem], 1, mem, pl.ds(0, 80), 0)
    for load in loads[1:]:
        load.wait()
    prepare(mem, dif_ref, mask_ref, val_ref, var_ref, cell_ref, blk_ref, aux, ob)
    for d in (0, 2):
        scatter_aux(d)
    forward(aux, 1, None, pl.ds(*NEED_AUX[1]), LEVELS)
    for dg in (0, 2):
        @when(~in_rows[dg])
        def _():
            for h in range(3):
                g_ref[h, dg] = jnp.zeros((LEVELS, 80, 128), F32)
                a_ref[h, dg] = jnp.ones((AUX, 128), F32)
    for h in (0, 2):
        @when(~in_sides[h // 2])
        def _():
            g_ref[h] = jnp.zeros((3, LEVELS, 80, 128), F32)
            a_ref[h] = jnp.ones((3, AUX, 128), F32)
    g_ref[1, 1, mem] = xs[mem]
    a_ref[1, 1] = aux[...]

    def arrival(dg, o):
        part = pl.ds(*NEED[dg])

        @when(in_rows[dg])
        def _():
            pltpu.make_async_remote_copy(
                src_ref=xs.at[0, part], dst_ref=g_ref.at[1, dg, back[o], part],
                send_sem=ssem.at[dg, o], recv_sem=rsem.at[dg, o],
                device_id=(mem, rows[dg], gy), device_id_type=MESH).wait_recv()
        if dg == 1:
            halo(g_ref.at[1, 1, back[o]], back[o], o)
        forward(g_ref.at[1, dg, back[o], part], dg, back[o], part, o)

    for o in (1, 3, 2):
        arrival(1, o)
    for dg in (0, 2):
        part = pl.ds(*NEED_AUX[dg])

        @when(in_rows[dg])
        def _():
            pltpu.make_async_remote_copy(
                src_ref=aux.at[part], dst_ref=a_ref.at[1, dg, part], send_sem=asem.at[dg], recv_sem=arsem.at[dg],
                device_id=(mem, rows[dg], gy), device_id_type=MESH).wait_recv()
        forward(a_ref.at[1, dg, part], dg, None, part, LEVELS)
    def passed_on(h, dg, chunks):
        @when(in_sides[h // 2], in_rows[dg])
        def _():
            for o in range(LEVELS) if chunks else ():
                part = pl.ds(*NEED[dg])
                pltpu.make_async_remote_copy(
                    src_ref=xs.at[0, part], dst_ref=g_ref.at[h, dg, back[o], part],
                    send_sem=fsem.at[0, dg, o], recv_sem=frsem.at[h // 2, dg, o],
                    device_id=(mem, gx, sides[0]), device_id_type=MESH).wait_recv()
            if not chunks:
                pltpu.make_async_remote_copy(
                    src_ref=aux.at[pl.ds(*NEED_AUX[dg])], dst_ref=a_ref.at[h, dg, pl.ds(*NEED_AUX[dg])],
                    send_sem=fsem.at[0, dg, LEVELS], recv_sem=frsem.at[h // 2, dg, LEVELS],
                    device_id=(mem, gx, sides[0]), device_id_type=MESH).wait_recv()

    weigh(ob, wc)
    for dg in (0, 2):
        arrival(dg, 0)
    for h in (0, 2):
        passed_on(h, 1, True)
        for dg in (1, 0, 2):
            passed_on(h, dg, False)
    assemble(grid, g_ref, a_ref, f0, dif, wet, (1,))
    forecast(f0, f1, dif, wet, pt, ((7, 10), 3), ((8, 10), 2))
    aim(grid, a_ref, hot, obs, wc)
    for o in (1, 3, 2):
        for dg in (0, 2):
            arrival(dg, o)
    for h in (0, 2):
        for dg in (0, 2):
            passed_on(h, dg, True)
    assemble(grid, g_ref, a_ref, f0, dif, wet, (0, 2))
    forecast(f0, f1, dif, wet, pt, ((1, 13), 6), ((2, 12), 6))
    def give_back(a):
        part = pl.ds(4 * a, 4)
        for o in (2, 1, 3):
            start(pltpu.make_async_remote_copy(
                src_ref=y_ref.at[there[o], :, part], dst_ref=out_ref.at[:, mem, part],
                send_sem=bsem.at[a, o], recv_sem=brsem.at[a, o],
                device_id=(there[o], gx, gy), device_id_type=MESH))

    analyse(grid, y_ref, give_back, pt, hot, obs, slab, wc, *scratch[9:])
    out_ref[:, mem] = y_ref[mem]
    for a in range(2):
        for o in range(1, LEVELS):
            part = pl.ds(4 * a, 4)
            pltpu.make_async_remote_copy(
                src_ref=y_ref.at[0, :, part], dst_ref=out_ref.at[:, back[o], part],
                send_sem=bsem.at[a, o], recv_sem=brsem.at[a, o],
                device_id=(there[o], gx, gy), device_id_type=MESH).wait_recv()
    for copy, conditions in sends:
        when(*conditions)(copy.wait_send)


def split(x):
    high = x.astype(jnp.bfloat16).astype(F32)
    return high, x - high


def mxu(a, b):
    return lax.dot_general(a, b, (((1,), (0,)), ((), ())), preferred_element_type=F32)


def mxu_nt(a, b):
    return lax.dot_general(a, b, (((1,), (1,)), ((), ())), preferred_element_type=F32)


def iota(shape, axis):
    return lax.broadcasted_iota(jnp.int32, shape, axis)


def block_of(lane):
    return jnp.where(lane < 40, 0, jnp.where(lane < 80, 1, jnp.where(lane < 120, 2, 3)))


def three_high(value, block):
    parts = [jnp.where(block == i, value, 0.0) for i in range(3)]
    return jnp.concatenate(parts + [jnp.zeros((8, value.shape[1]), F32)], axis=0)


def masks(n_gx, n_gy):
    gx, gy = lax.axis_index("gx"), lax.axis_index("gy")
    one = lambda c: jnp.where(c, 1.0, 0.0).astype(F32)
    lane1 = iota((1, 128), 1)
    in_grid = (one(gx > 0), jnp.float32(1.0), one(gx < n_gx - 1))
    return in_grid, jnp.where(lane1 < 64, one(gy < n_gy - 1), one(gy > 0)), lane1


def weigh(ob_ref, wc):
    third = lax.rem(iota((1, 384), 1) >> 4, 3)
    for a in range(2):
        for r in range(3):
            near = []
            for c in range(3):
                code = 3 * r + c
                taper = 1.0 if code == 4 else 0.5 if (r == 1 or c == 1) else 0.25
                chosen = jnp.zeros((1, 256), F32)
                for s in range(5):
                    blocks = ob_ref[5 * a + s:5 * a + s + 1, :]
                    chosen = chosen + jnp.where(blocks == code, taper, 0.0)
                chosen = jnp.concatenate([chosen, jnp.zeros((1, 128), F32)], axis=1)
                near.append(pltpu.roll(chosen, (16 * (c - 1)) % 384, 1) if c != 1 else chosen)
            for i in range(3):
                which = lax.rem(third + 4 - i, 3)
                wc[a, 3 * r + i:3 * r + i + 1, :] = jnp.where(
                    which == 0, near[0], jnp.where(which == 1, near[1], near[2]))


def assemble(grid, g_ref, a_ref, f0, dif, wet, groups):
    in_grid, beside, lane1 = grid

    def both(h_of, dg):
        own, side = h_of(1), jnp.where(lane1 < 64, h_of(2), h_of(0)) * (beside * in_grid[dg])
        return (own if dg == 1 else own * in_grid[dg]), side

    for t in range(20):
        dg, r = (0, t + 2) if t < 6 else (1, t - 6) if t < 14 else (2, t - 14)
        if dg not in groups:
            continue
        main, rest = MAIN[r], REST[r]
        for s in range(LEVELS):
            own, side = both(lambda h: g_ref[h, dg, s, main:main + 8, :], dg)
            f0[t, 8 * s:8 * s + 8, 0:128] = own
            f0[t, 8 * s:8 * s + 8, 128:256] = side
            own, side = both(lambda h: g_ref[h, dg, s, rest:rest + 2, :], dg)
            f0[t, 32 + 2 * s:34 + 2 * s, 0:128] = own
            f0[t, 32 + 2 * s:34 + 2 * s, 128:256] = side
        own, side = both(lambda h: a_ref[h, dg, FLOW[r]:FLOW[r] + 1, :], dg)
        dif[t, :, 0:128] = own
        dif[t, :, 128:256] = side
        own, side = both(lambda h: a_ref[h, dg, WET[r]:WET[r] + 1, :], dg)
        wet[t, :, 0:128] = own
        wet[t, :, 128:256] = side


def advance(src, dif, wet, t):
    c = src[t]
    around = src[t + 1] + src[t - 1]
    around = around + pltpu.roll(c, 255, 1) + pltpu.roll(c, 1, 1)
    return wet[t] * (c + dif[t] * (around - 4.0 * c))


def forecast(f0, f1, dif, wet, pt, first, second):
    def one(k, carry):
        for low in first[0]:
            f1[low + k] = advance(f0, dif, wet, low + k)
        return carry

    lax.fori_loop(0, first[1], one, 0)

    def two(k, carry):
        for low in second[0]:
            value = advance(f1, dif, wet, low + k)
            m = jnp.sum(value, axis=0, keepdims=True) / MEMBERS
            pt[low + k - 2, 0:40, :] = value - m
            pt[low + k - 2, 40:48, :] = jnp.where(iota((8, 256), 0) == 0, m, 0.0)
        return carry

    lax.fori_loop(0, second[1], two, 0)


def aim(grid, a_ref, hot, obs, wc):
    in_grid, beside, lane1 = grid
    lane2 = iota((1, 256), 1)
    for p in range(4):
        dg, a = ((0, 1), (1, 0), (1, 1), (2, 0))[p]

        def rows_of(kind):
            at = SEEN[a] + 2 * kind
            own = jnp.concatenate([a_ref[1, dg, at:at + 1, :], a_ref[1, dg, at + 1:at + 2, :]], axis=1)
            return own, jnp.where(lane1 < 64, a_ref[2, dg, at:at + 1, :], a_ref[0, dg, at + 1:at + 2, :])

        value, variance, cell = rows_of(0), rows_of(1), rows_of(2)
        for k, (lane, shift) in enumerate(((lane2, 0), (lane1, jnp.where(lane1 < 64, 0, 64)))):
            c = cell[k].astype(jnp.int32)
            target = (c >> 3) * 128 + ((lane >> 4) << 3) + (c & 7) + shift
            at, width = 256 * k, lane.shape[1]

            def fill(n, carry):
                top = pl.multiple_of(n * 64, 64)
                hot[p, pl.ds(top, 64), at:at + width] = jnp.where(
                    iota((64, width), 0) == target - n * 64, 1.0, 0.0).astype(F32)
                return carry

            lax.fori_loop(0, 8, fill, 0)
        obs[p:p + 1, :] = jnp.concatenate(value, axis=1)
        inside = jnp.concatenate([jnp.ones((1, 256), F32), beside], axis=1) * in_grid[dg]
        obs[4 + p:5 + p, :] = inside / jnp.concatenate(variance, axis=1)
    for a in range(2):
        for r in range(3):
            p = a + r
            rows = wc[a, 3 * r:3 * r + 3, :] * obs[4 + p:5 + p, :]
            wc[a, 3 * r:3 * r + 3, :] = pltpu.roll(rows, 80 * (p % 3), 1) if p % 3 else rows


GROUPS = 11


def analyse(grid, y_ref, done, pt, hot, obs, slab, wc, gram, tr, tv, ps, zs):
    lane1 = grid[2]

    for p in range(4):
        found = []
        for k, (low, high) in enumerate(((0, 256), (256, 384))):
            rows = jnp.concatenate([pt[4 * p + r, :, 128 * k:128 * k + 128] for r in range(4)], axis=1)
            both_parts = mxu(jnp.concatenate(split(rows), axis=0), hot[p, :, low:high])
            found.append(both_parts[0:48] + both_parts[48:96])
        whole = jnp.concatenate(found, axis=1)
        tail = jnp.where(iota((8, 384), 0) == 0, obs[p:p + 1, :] - whole[40:48], 0.0)
        whole = jnp.concatenate([whole[0:40], tail], axis=0)
        slab[p] = pltpu.roll(whole, 80 * (p % 3), 1) if p % 3 else whole

    lane2 = iota((1, 256), 1)
    part = jnp.where(lane2 < 80, 0, jnp.where(lane2 < 160, 1, jnp.where(lane2 < 240, 2, 3)))
    slot = (lane2 - 80 * part) >> 4
    block = block_of(lane1)
    diagonal = (lane1 - 40 * block == iota((40, 128), 0)) & (lane1 < 120)

    def keep(n, o):
        system = jnp.where(diagonal, 1.0, 0.0) + o[0:40] / (MEMBERS - 1.0)
        gram[n, 0:40, :] = system
        gram[n, 40:48, :] = o[40:48] / (MEMBERS - 1.0)
        tr[n:n + 1, :] = jnp.sum(jnp.where(diagonal, system, 0.0), axis=0, keepdims=True)

    last = []
    for g in range(6):
        turn = (16 - 48 * g) % 384

        def window(x):
            return pltpu.roll(x, turn, 1)[:, 0:256]

        parts = [window(slab[p]) for p in range(4)]
        for a in range(2):
            left = jnp.where(part == 0, parts[3 * a], jnp.where(part == 1, parts[1], parts[2]))
            weights = window(wc[a])
            right = []
            for i in range(3):
                w = jnp.zeros((1, 256), F32)
                for r in range(3):
                    w = jnp.where(part == (a + r) % 3, weights[3 * r + i:3 * r + i + 1], w)
                w = jnp.where((part < 3) & (slot >= i) & (slot <= i + 2), w, 0.0)
                right.append(left[0:40] * w)
            right.append(jnp.zeros((8, 256), F32))
            right = jnp.concatenate(right, axis=0)
            o = mxu_nt(jnp.concatenate(split(left), axis=0), jnp.concatenate(split(right), axis=0))
            o = o[0:48] + o[48:96]
            o = o[:, 0:128] + o[:, 128:256]
            if g < 5:
                keep(2 * g + a, o)
            else:
                last.append(o)
    keep(10, jnp.where(block == 0, last[0], jnp.where(block == 1, pltpu.roll(last[1], 40, 1), 0.0)))
    tr[11:12, :] = jnp.ones((1, 128), F32)

    rows = tr[...]
    sums = [jnp.sum(jnp.where(block == i, rows, 0.0), axis=1, keepdims=True) for i in range(3)]
    tv[...] = jnp.where(block == 0, sums[0], jnp.where(block == 1, sums[1], sums[2]))
    for n in range(GROUPS):
        ps[n] = gram[n, 0:40, :] / tv[n:n + 1, :]
        zs[n] = jnp.where(diagonal, 1.0, 0.0)

    wide = jnp.concatenate([block, block], axis=1)

    def times(rows_of, stacked, by_rows):
        count = len(rows_of)
        if by_rows:
            o = mxu(jnp.concatenate([x for v in rows_of for x in split(v)], axis=0), stacked)
            o = [o[80 * k:80 * k + 40] + o[80 * k + 40:80 * k + 80] for k in range(count)]
        else:
            o = mxu(jnp.concatenate([jnp.concatenate(split(v), axis=1) for v in rows_of], axis=0),
                    jnp.concatenate([stacked, stacked], axis=0))
            o = [o[40 * k:40 * k + 40] for k in range(count)]
        return [x[:, 0:128] + x[:, 128:256] for x in o]

    def sweep(step, carry):
        for n in range(GROUPS):
            p, z = ps[n], zs[n]
            stacked = three_high(jnp.concatenate(split(p), axis=1), wide)
            pp, zp = times([p, z], stacked, BY_ROWS[0])
            zs[n] = 1.5 * z - 0.5 * zp
            q = 1.5 * p - 0.5 * pp
            ps[n] = 1.5 * q - 0.5 * times([q], stacked, BY_ROWS[1])[0]
        return carry

    lax.fori_loop(0, NS_ITERS - 1, sweep, 0)

    ones = jnp.where((block_of(iota((128, 128), 0)) == block) & (lane1 < 120), 1.0, 0.0).astype(F32)
    spreads, columns = [], []
    for n in range(GROUPS):
        z = zs[n]
        stacked = three_high(jnp.concatenate(split(ps[n]), axis=1), wide)
        z = 1.5 * z - 0.5 * times([z], stacked, BY_ROWS[2])[0]
        spreads.append(z / jnp.sqrt(tv[n:n + 1, :]))
        columns.append(jnp.concatenate(split(spreads[n] * gram[n, 40:41, :]), axis=1))
    partial = mxu(jnp.concatenate(columns, axis=0), jnp.concatenate([ones, ones], axis=0))
    transforms = []
    for n in range(GROUPS):
        centre = jnp.sum(spreads[n] * partial[40 * n:40 * n + 40], axis=0, keepdims=True)
        th, tl = split(spreads[n] + centre)
        transforms.append(jnp.concatenate([
            jnp.concatenate([th, th], axis=1), jnp.concatenate([tl, jnp.zeros_like(tl)], axis=1)], axis=0))

    patch = lax.rem(iota((1, 512), 1), 128) >> 3
    flat = y_ref.reshape(MEMBERS * 8, 128)
    for a in range(2):
        here = jnp.concatenate([pt[4 + 4 * a + r, 0:40, 0:128] for r in range(4)], axis=1)
        here = split(here)
        total = jnp.zeros((80, 512), F32)
        for g in range(6):
            n = 2 * g + a if g < 5 else 10
            ids = (3 * g, 3 * g + 1, 3 * g + 2) if g < 5 else (15, -1, -1) if a == 0 else (-1, 15, -1)
            pieces = []
            for v in here:
                pieces += [jnp.where(patch == c, v, 0.0) if c >= 0 else jnp.zeros((40, 512), F32) for c in ids]
                pieces.append(jnp.zeros((8, 512), F32))
            total = total + mxu(transforms[n], jnp.concatenate(pieces, axis=0))
        total = total[0:40] + total[40:80]
        for r in range(4):
            value = total[:, 128 * r:128 * r + 128] + pt[4 + 4 * a + r, 40:41, 0:128]
            for s in range(LEVELS):
                flat[pl.ds(80 * s + 4 * a + r, 8, stride=8), :] = value[8 * s:8 * s + 8]
                flat[pl.ds(80 * s + 64 + 4 * a + r, 2, stride=8), :] = value[32 + 2 * s:34 + 2 * s]
        done(a)


def compute_kernel(n_gx, n_gy, g_ref, a_ref, ob, y_ref, f0, f1, dif, wet, pt, hot, obs, slab, wc, *rest):
    grid = masks(n_gx, n_gy)
    weigh(ob, wc)
    aim(grid, a_ref, hot, obs, wc)
    assemble(grid, g_ref, a_ref, f0, dif, wet, (1,))
    forecast(f0, f1, dif, wet, pt, ((7, 10), 3), ((8, 10), 2))
    assemble(grid, g_ref, a_ref, f0, dif, wet, (0, 2))
    forecast(f0, f1, dif, wet, pt, ((1, 13), 6), ((2, 12), 6))
    analyse(grid, y_ref, lambda a: None, pt, hot, obs, slab, wc, *rest)


def scratch_of():
    return [
        pltpu.VMEM((20, 40, 256), F32), pltpu.VMEM((20, 40, 256), F32),
        pltpu.VMEM((20, 1, 256), F32), pltpu.VMEM((20, 1, 256), F32),
        pltpu.VMEM((16, 48, 256), F32), pltpu.VMEM((4, 512, 384), F32), pltpu.VMEM((8, 384), F32),
        pltpu.VMEM((4, 48, 384), F32), pltpu.VMEM((2, 16, 384), F32),
        pltpu.VMEM((12, 48, 128), F32), pltpu.VMEM((12, 128), F32), pltpu.VMEM((12, 128), F32),
        pltpu.VMEM((12, 40, 128), F32), pltpu.VMEM((12, 40, 128), F32)]


def solution(mesh):
    n_gx, n_gy = mesh.shape["gx"], mesh.shape["gy"]
    dma = pltpu.SemaphoreType.DMA

    def local(*args):
        def body(*refs):
            cycle_kernel(n_gx, n_gy, *refs)

        return pl.pallas_call(
            body, out_shape=jax.ShapeDtypeStruct((OWN, LEVELS, 8, 128), F32),
            in_specs=[pl.BlockSpec(memory_space=pl.ANY)] * 7, out_specs=pl.BlockSpec(memory_space=pltpu.VMEM),
            scratch_shapes=[pltpu.VMEM(a.shape, a.dtype) for a in args] + [
                pltpu.VMEM((LEVELS, 80, 128), F32), pltpu.VMEM((AUX, 128), F32), pltpu.VMEM((16, 256), F32),
                pltpu.VMEM((3, 3, LEVELS, 80, 128), F32), pltpu.VMEM((3, 3, AUX, 128), F32),
                pltpu.VMEM((LEVELS, OWN, 8, 128), F32)] + scratch_of() + [
                dma((3, LEVELS)), dma((3, LEVELS)), dma((3,)), dma((3,)),
                dma((2, 3, LEVELS + 1)), dma((2, 3, LEVELS + 1)), dma((7,)), dma((2, LEVELS)), dma((2, LEVELS))],
            compiler_params=pltpu.CompilerParams(collective_id=0, has_side_effects=True),
            name="cycle")(*args)

    return jax.shard_map(
        local,
        mesh=mesh,
        in_specs=(
            P("mem", None, "gx", "gy"),
            P(None, "gx", "gy"),
            P("gx", "gy"),
            P(None, None, "gx", "gy"),
            P(None, None, "gx", "gy"),
            P(None, None, "gx", "gy"),
            P(None, "gx", "gy"),
        ),
        out_specs=P("mem", None, "gx", "gy"),
        check_vma=False,
    )
```

```python
import jax
import jax.numpy as jnp
from jax import lax
from jax.experimental import pallas as pl
from jax.experimental.pallas import tpu as pltpu
from jax.sharding import PartitionSpec as P

MESH = pl.DeviceIdType.MESH
F32 = jnp.float32
NS_ITERS = 7
BY_ROWS = (False, False, False)
SWEEP_UNROLL = 6
FORECAST_UNROLL = 2
LEVELS = 4
OWN = 10
MEMBERS = 40
OBS = 16
MAIN = (64, 72, 20, 28, 36, 44, 0, 8)
REST = (60, 62, 52, 54, 56, 58, 16, 18)
AUX = 28
FLOW = (6, 7, 10, 11, 12, 13, 18, 19)
WET = (8, 9, 14, 15, 16, 17, 20, 21)
SEEN = (0, 22)
NEED = ((0, 60), (0, 80), (20, 60))
NEED_AUX = ((10, 18), (0, 28), (0, 18))


def neighbours(n_gx, n_gy):
    mem, gx, gy = lax.axis_index("mem"), lax.axis_index("gx"), lax.axis_index("gy")
    rows = (lax.rem(gx + n_gx - 1, n_gx), gx, lax.rem(gx + 1, n_gx))
    sides = (lax.rem(gy + n_gy - 1, n_gy), lax.rem(gy + 1, n_gy))
    there = [lax.rem(mem + o, LEVELS) for o in range(LEVELS)]
    back = [lax.rem(mem + LEVELS - o, LEVELS) for o in range(LEVELS)]
    return mem, gx, gy, rows, sides, there, back


def lay_out(x_ref, xs):
    flat = x_ref.reshape(OWN * LEVELS * 8, 128)
    for k in range(LEVELS):
        for r in range(8):
            xs[k, MAIN[r]:MAIN[r] + 8, :] = flat[pl.ds(k * 8 + r, 8, stride=32), :]
            xs[k, REST[r]:REST[r] + 2, :] = flat[pl.ds(256 + k * 8 + r, 2, stride=32), :]


def prepare(level, dif_ref, mask_ref, val_ref, var_ref, cell_ref, blk_ref, aux, ob):
    for rows, value in ((FLOW, dif_ref[level]), (WET, mask_ref[...].astype(F32))):
        for r in range(8):
            aux[rows[r]:rows[r] + 1, :] = value[r:r + 1]
    spread_out = jnp.where(iota((16, 256), 0) == iota((16, 256), 1) >> 4, 1.0, 0.0).astype(F32)
    kinds = [ref[level].astype(F32) for ref in (val_ref, var_ref, cell_ref)]
    stacked = jnp.concatenate([kinds[k][:, a, :] for a in range(2) for k in range(3)], axis=0)
    wide = lax.dot_general(stacked, spread_out, (((1,), (0,)), ((), ())), precision=lax.Precision.HIGHEST,
                           preferred_element_type=F32)
    mine = iota((16, 256), 0) == (iota((16, 256), 1) & 15)
    for n in range(6):
        row = jnp.sum(jnp.where(mine, wide[16 * n:16 * n + 16], 0.0), axis=0, keepdims=True)
        at = SEEN[n // 3] + 2 * (n % 3)
        aux[at:at + 1, :] = row[:, 0:128]
        aux[at + 1:at + 2, :] = row[:, 128:256]
    blocks = blk_ref[...].astype(F32)
    blocks = jnp.concatenate([blocks[:, a, :] for a in range(2)] + [jnp.zeros((6, 16), F32)], axis=0)
    ob[...] = mxu(blocks, spread_out)


def cycle_kernel(n_gx, n_gy, x_any, dif_any, mask_any, val_any, var_any, cell_any, blk_any, out_ref,
                 x_ref, dif_ref, mask_ref, val_ref, var_ref, cell_ref, blk_ref, xs, aux, ob, g_ref, a_ref, y_ref, *rest):
    scratch, (ssem, rsem, asem, arsem, fsem, frsem, lsem, bsem, brsem) = rest[:-9], rest[-9:]
    mem, gx, gy, rows, sides, there, back = neighbours(n_gx, n_gy)

    in_rows = (gx > 0, None, gx < n_gx - 1)
    in_sides = (gy > 0, gy < n_gy - 1)

    def when(*conditions):
        known = [c for c in conditions if c is not None]
        if not known:
            return lambda f: f()
        return pl.when(known[0] if len(known) == 1 else known[0] & known[1])

    barrier = pltpu.get_barrier_semaphore()
    count = LEVELS - 1
    for d in range(3):
        @when(in_rows[d])
        def _():
            for o in range(1, LEVELS) if d == 1 else (0,):
                pl.semaphore_signal(barrier, inc=1, device_id=(there[o], rows[d], gy), device_id_type=MESH)
        if d != 1:
            count = count + jnp.where(in_rows[d], 1, 0)
    for e in range(2):
        @when(in_sides[e])
        def _():
            pl.semaphore_signal(barrier, inc=1, device_id=(mem, gx, sides[e]), device_id_type=MESH)
        count = count + jnp.where(in_sides[e], 1, 0)

    loads = [pltpu.make_async_copy(src, dst, lsem.at[n]) for n, (src, dst) in enumerate((
        (x_any, x_ref), (dif_any, dif_ref), (mask_any, mask_ref), (val_any, val_ref), (var_any, var_ref),
        (cell_any, cell_ref), (blk_any, blk_ref)))]
    for load in loads:
        load.start()
    loads[0].wait()
    lay_out(x_ref, xs)
    f0, f1, dif, wet, pt, hot, obs, slab, wc = scratch[:9]
    grid = masks(n_gx, n_gy)
    pl.semaphore_wait(barrier, count)

    sends = []

    def start(copy, *conditions):
        when(*conditions)(copy.start)
        sends.append((copy, conditions))

    def forward(source, dg, slot, part, index):
        for e, side in enumerate(sides):
            h = 2 if e == 0 else 0
            dst = a_ref.at[h, dg, part] if slot is None else g_ref.at[h, dg, slot, part]
            start(pltpu.make_async_remote_copy(
                src_ref=source, dst_ref=dst, send_sem=fsem.at[e, dg, index], recv_sem=frsem.at[h // 2, dg, index],
                device_id=(mem, gx, side), device_id_type=MESH), in_rows[dg], in_sides[e])

    def scatter(o):
        start(pltpu.make_async_remote_copy(
            src_ref=xs.at[there[o]], dst_ref=g_ref.at[1, 1, mem], send_sem=ssem.at[1, o], recv_sem=rsem.at[1, o],
            device_id=(there[o], gx, gy), device_id_type=MESH))

    def halo(source, slot, o):
        for d in (0, 2):
            part = pl.ds(*NEED[2 - d])
            start(pltpu.make_async_remote_copy(
                src_ref=source.at[part], dst_ref=g_ref.at[1, 2 - d, slot, part],
                send_sem=ssem.at[d, o], recv_sem=rsem.at[2 - d, o],
                device_id=(mem, rows[d], gy), device_id_type=MESH), in_rows[d])

    def scatter_aux(d):
        part = pl.ds(*NEED_AUX[2 - d])
        start(pltpu.make_async_remote_copy(
            src_ref=aux.at[part], dst_ref=a_ref.at[1, 2 - d, part], send_sem=asem.at[d], recv_sem=arsem.at[2 - d],
            device_id=(mem, rows[d], gy), device_id_type=MESH), in_rows[d])

    for o in (2, 1, 3):
        scatter(o)
    halo(xs.at[mem], mem, 0)
    forward(xs.at[mem], 1, mem, pl.ds(0, 80), 0)
    for load in loads[1:]:
        load.wait()
    prepare(mem, dif_ref, mask_ref, val_ref, var_ref, cell_ref, blk_ref, aux, ob)
    for d in (0, 2):
        scatter_aux(d)
    forward(aux, 1, None, pl.ds(*NEED_AUX[1]), LEVELS)
    for dg in (0, 2):
        @when(~in_rows[dg])
        def _():
            for h in range(3):
                g_ref[h, dg] = jnp.zeros((LEVELS, 80, 128), F32)
                a_ref[h, dg] = jnp.ones((AUX, 128), F32)
    for h in (0, 2):
        @when(~in_sides[h // 2])
        def _():
            g_ref[h] = jnp.zeros((3, LEVELS, 80, 128), F32)
            a_ref[h] = jnp.ones((3, AUX, 128), F32)
    g_ref[1, 1, mem] = xs[mem]
    a_ref[1, 1] = aux[...]

    def arrival(dg, o):
        part = pl.ds(*NEED[dg])

        @when(in_rows[dg])
        def _():
            pltpu.make_async_remote_copy(
                src_ref=xs.at[0, part], dst_ref=g_ref.at[1, dg, back[o], part],
                send_sem=ssem.at[dg, o], recv_sem=rsem.at[dg, o],
                device_id=(mem, rows[dg], gy), device_id_type=MESH).wait_recv()
        if dg == 1:
            halo(g_ref.at[1, 1, back[o]], back[o], o)
        forward(g_ref.at[1, dg, back[o], part], dg, back[o], part, o)

    for o in (1, 3, 2):
        arrival(1, o)
    for dg in (0, 2):
        part = pl.ds(*NEED_AUX[dg])

        @when(in_rows[dg])
        def _():
            pltpu.make_async_remote_copy(
                src_ref=aux.at[part], dst_ref=a_ref.at[1, dg, part], send_sem=asem.at[dg], recv_sem=arsem.at[dg],
                device_id=(mem, rows[dg], gy), device_id_type=MESH).wait_recv()
        forward(a_ref.at[1, dg, part], dg, None, part, LEVELS)
    def passed_on(h, dg, chunks):
        @when(in_sides[h // 2], in_rows[dg])
        def _():
            for o in range(LEVELS) if chunks else ():
                part = pl.ds(*NEED[dg])
                pltpu.make_async_remote_copy(
                    src_ref=xs.at[0, part], dst_ref=g_ref.at[h, dg, back[o], part],
                    send_sem=fsem.at[0, dg, o], recv_sem=frsem.at[h // 2, dg, o],
                    device_id=(mem, gx, sides[0]), device_id_type=MESH).wait_recv()
            if not chunks:
                pltpu.make_async_remote_copy(
                    src_ref=aux.at[pl.ds(*NEED_AUX[dg])], dst_ref=a_ref.at[h, dg, pl.ds(*NEED_AUX[dg])],
                    send_sem=fsem.at[0, dg, LEVELS], recv_sem=frsem.at[h // 2, dg, LEVELS],
                    device_id=(mem, gx, sides[0]), device_id_type=MESH).wait_recv()

    weigh(ob, wc)
    for dg in (0, 2):
        arrival(dg, 0)
    for h in (0, 2):
        passed_on(h, 1, True)
        for dg in (1, 0, 2):
            passed_on(h, dg, False)
    assemble(grid, g_ref, a_ref, f0, dif, wet, (1,))
    forecast(f0, f1, dif, wet, pt, ((7, 10), 3), ((8, 10), 2))
    aim(grid, a_ref, hot, obs, wc)
    for o in (1, 3, 2):
        for dg in (0, 2):
            arrival(dg, o)
    for h in (0, 2):
        for dg in (0, 2):
            passed_on(h, dg, True)
    assemble(grid, g_ref, a_ref, f0, dif, wet, (0, 2))
    forecast(f0, f1, dif, wet, pt, ((1, 13), 6), ((2, 12), 6))
    def give_back(a):
        part = pl.ds(4 * a, 4)
        for o in (2, 1, 3):
            start(pltpu.make_async_remote_copy(
                src_ref=y_ref.at[there[o], :, part], dst_ref=out_ref.at[:, mem, part],
                send_sem=bsem.at[a, o], recv_sem=brsem.at[a, o],
                device_id=(there[o], gx, gy), device_id_type=MESH))

    analyse(grid, y_ref, give_back, pt, hot, obs, slab, wc, *scratch[9:])
    out_ref[:, mem] = y_ref[mem]
    for a in range(2):
        for o in range(1, LEVELS):
            part = pl.ds(4 * a, 4)
            pltpu.make_async_remote_copy(
                src_ref=y_ref.at[0, :, part], dst_ref=out_ref.at[:, back[o], part],
                send_sem=bsem.at[a, o], recv_sem=brsem.at[a, o],
                device_id=(there[o], gx, gy), device_id_type=MESH).wait_recv()
    for copy, conditions in sends:
        when(*conditions)(copy.wait_send)


def split(x):
    high = x.astype(jnp.bfloat16).astype(F32)
    return high, x - high


def mxu(a, b):
    return lax.dot_general(a, b, (((1,), (0,)), ((), ())), preferred_element_type=F32)


def mxu_nt(a, b):
    return lax.dot_general(a, b, (((1,), (1,)), ((), ())), preferred_element_type=F32)


def iota(shape, axis):
    return lax.broadcasted_iota(jnp.int32, shape, axis)


def block_of(lane):
    return jnp.where(lane < 40, 0, jnp.where(lane < 80, 1, jnp.where(lane < 120, 2, 3)))


def three_high(value, block):
    parts = [jnp.where(block == i, value, 0.0) for i in range(3)]
    return jnp.concatenate(parts + [jnp.zeros((8, value.shape[1]), F32)], axis=0)


def masks(n_gx, n_gy):
    gx, gy = lax.axis_index("gx"), lax.axis_index("gy")
    one = lambda c: jnp.where(c, 1.0, 0.0).astype(F32)
    lane1 = iota((1, 128), 1)
    in_grid = (one(gx > 0), jnp.float32(1.0), one(gx < n_gx - 1))
    return in_grid, jnp.where(lane1 < 64, one(gy < n_gy - 1), one(gy > 0)), lane1


def weigh(ob_ref, wc):
    third = lax.rem(iota((1, 384), 1) >> 4, 3)
    for a in range(2):
        for r in range(3):
            near = []
            for c in range(3):
                code = 3 * r + c
                taper = 1.0 if code == 4 else 0.5 if (r == 1 or c == 1) else 0.25
                chosen = jnp.zeros((1, 256), F32)
                for s in range(5):
                    blocks = ob_ref[5 * a + s:5 * a + s + 1, :]
                    chosen = chosen + jnp.where(blocks == code, taper, 0.0)
                chosen = jnp.concatenate([chosen, jnp.zeros((1, 128), F32)], axis=1)
                near.append(pltpu.roll(chosen, (16 * (c - 1)) % 384, 1) if c != 1 else chosen)
            for i in range(3):
                which = lax.rem(third + 4 - i, 3)
                wc[a, 3 * r + i:3 * r + i + 1, :] = jnp.where(
                    which == 0, near[0], jnp.where(which == 1, near[1], near[2]))


def assemble(grid, g_ref, a_ref, f0, dif, wet, groups):
    in_grid, beside, lane1 = grid

    def both(h_of, dg):
        own, side = h_of(1), jnp.where(lane1 < 64, h_of(2), h_of(0)) * (beside * in_grid[dg])
        return (own if dg == 1 else own * in_grid[dg]), side

    for t in range(20):
        dg, r = (0, t + 2) if t < 6 else (1, t - 6) if t < 14 else (2, t - 14)
        if dg not in groups:
            continue
        main, rest = MAIN[r], REST[r]
        for s in range(LEVELS):
            own, side = both(lambda h: g_ref[h, dg, s, main:main + 8, :], dg)
            f0[t, 8 * s:8 * s + 8, 0:128] = own
            f0[t, 8 * s:8 * s + 8, 128:256] = side
            own, side = both(lambda h: g_ref[h, dg, s, rest:rest + 2, :], dg)
            f0[t, 32 + 2 * s:34 + 2 * s, 0:128] = own
            f0[t, 32 + 2 * s:34 + 2 * s, 128:256] = side
        own, side = both(lambda h: a_ref[h, dg, FLOW[r]:FLOW[r] + 1, :], dg)
        dif[t, :, 0:128] = own
        dif[t, :, 128:256] = side
        own, side = both(lambda h: a_ref[h, dg, WET[r]:WET[r] + 1, :], dg)
        wet[t, :, 0:128] = own
        wet[t, :, 128:256] = side


def advance(src, dif, wet, t):
    c = src[t]
    around = src[t + 1] + src[t - 1]
    around = around + pltpu.roll(c, 255, 1) + pltpu.roll(c, 1, 1)
    return wet[t] * (c + dif[t] * (around - 4.0 * c))


def forecast(f0, f1, dif, wet, pt, first, second):
    def one(k, carry):
        for low in first[0]:
            f1[low + k] = advance(f0, dif, wet, low + k)
        return carry

    lax.fori_loop(0, first[1], one, 0, unroll=FORECAST_UNROLL)

    def two(k, carry):
        for low in second[0]:
            value = advance(f1, dif, wet, low + k)
            m = jnp.sum(value, axis=0, keepdims=True) / MEMBERS
            pt[low + k - 2, 0:40, :] = value - m
            pt[low + k - 2, 40:48, :] = jnp.where(iota((8, 256), 0) == 0, m, 0.0)
        return carry

    lax.fori_loop(0, second[1], two, 0, unroll=FORECAST_UNROLL)


def aim(grid, a_ref, hot, obs, wc):
    in_grid, beside, lane1 = grid
    lane2 = iota((1, 256), 1)
    for p in range(4):
        dg, a = ((0, 1), (1, 0), (1, 1), (2, 0))[p]

        def rows_of(kind):
            at = SEEN[a] + 2 * kind
            own = jnp.concatenate([a_ref[1, dg, at:at + 1, :], a_ref[1, dg, at + 1:at + 2, :]], axis=1)
            return own, jnp.where(lane1 < 64, a_ref[2, dg, at:at + 1, :], a_ref[0, dg, at + 1:at + 2, :])

        value, variance, cell = rows_of(0), rows_of(1), rows_of(2)
        for k, (lane, shift) in enumerate(((lane2, 0), (lane1, jnp.where(lane1 < 64, 0, 64)))):
            c = cell[k].astype(jnp.int32)
            target = (c >> 3) * 128 + ((lane >> 4) << 3) + (c & 7) + shift
            at, width = 256 * k, lane.shape[1]

            def fill(n, carry):
                top = pl.multiple_of(n * 64, 64)
                hot[p, pl.ds(top, 64), at:at + width] = jnp.where(
                    iota((64, width), 0) == target - n * 64, 1.0, 0.0).astype(F32)
                return carry

            lax.fori_loop(0, 8, fill, 0)
        obs[p:p + 1, :] = jnp.concatenate(value, axis=1)
        inside = jnp.concatenate([jnp.ones((1, 256), F32), beside], axis=1) * in_grid[dg]
        obs[4 + p:5 + p, :] = inside / jnp.concatenate(variance, axis=1)
    for a in range(2):
        for r in range(3):
            p = a + r
            rows = wc[a, 3 * r:3 * r + 3, :] * obs[4 + p:5 + p, :]
            wc[a, 3 * r:3 * r + 3, :] = pltpu.roll(rows, 80 * (p % 3), 1) if p % 3 else rows


GROUPS = 11


def analyse(grid, y_ref, done, pt, hot, obs, slab, wc, gram, tr, tv, ps, zs):
    lane1 = grid[2]

    for p in range(4):
        found = []
        for k, (low, high) in enumerate(((0, 256), (256, 384))):
            rows = jnp.concatenate([pt[4 * p + r, :, 128 * k:128 * k + 128] for r in range(4)], axis=1)
            both_parts = mxu(jnp.concatenate(split(rows), axis=0), hot[p, :, low:high])
            found.append(both_parts[0:48] + both_parts[48:96])
        whole = jnp.concatenate(found, axis=1)
        tail = jnp.where(iota((8, 384), 0) == 0, obs[p:p + 1, :] - whole[40:48], 0.0)
        whole = jnp.concatenate([whole[0:40], tail], axis=0)
        slab[p] = pltpu.roll(whole, 80 * (p % 3), 1) if p % 3 else whole

    lane2 = iota((1, 256), 1)
    part = jnp.where(lane2 < 80, 0, jnp.where(lane2 < 160, 1, jnp.where(lane2 < 240, 2, 3)))
    slot = (lane2 - 80 * part) >> 4
    block = block_of(lane1)
    diagonal = (lane1 - 40 * block == iota((40, 128), 0)) & (lane1 < 120)

    def keep(n, o):
        system = jnp.where(diagonal, 1.0, 0.0) + o[0:40] / (MEMBERS - 1.0)
        gram[n, 0:40, :] = system
        gram[n, 40:48, :] = o[40:48] / (MEMBERS - 1.0)
        tr[n:n + 1, :] = jnp.sum(jnp.where(diagonal, system, 0.0), axis=0, keepdims=True)

    last = []
    for g in range(6):
        turn = (16 - 48 * g) % 384

        def window(x):
            return pltpu.roll(x, turn, 1)[:, 0:256]

        parts = [window(slab[p]) for p in range(4)]
        for a in range(2):
            left = jnp.where(part == 0, parts[3 * a], jnp.where(part == 1, parts[1], parts[2]))
            weights = window(wc[a])
            right = []
            for i in range(3):
                w = jnp.zeros((1, 256), F32)
                for r in range(3):
                    w = jnp.where(part == (a + r) % 3, weights[3 * r + i:3 * r + i + 1], w)
                w = jnp.where((part < 3) & (slot >= i) & (slot <= i + 2), w, 0.0)
                right.append(left[0:40] * w)
            right.append(jnp.zeros((8, 256), F32))
            right = jnp.concatenate(right, axis=0)
            o = mxu_nt(jnp.concatenate(split(left), axis=0), jnp.concatenate(split(right), axis=0))
            o = o[0:48] + o[48:96]
            o = o[:, 0:128] + o[:, 128:256]
            if g < 5:
                keep(2 * g + a, o)
            else:
                last.append(o)
    keep(10, jnp.where(block == 0, last[0], jnp.where(block == 1, pltpu.roll(last[1], 40, 1), 0.0)))
    tr[11:12, :] = jnp.ones((1, 128), F32)

    rows = tr[...]
    sums = [jnp.sum(jnp.where(block == i, rows, 0.0), axis=1, keepdims=True) for i in range(3)]
    tv[...] = jnp.where(block == 0, sums[0], jnp.where(block == 1, sums[1], sums[2]))
    for n in range(GROUPS):
        ps[n] = gram[n, 0:40, :] / tv[n:n + 1, :]
        zs[n] = jnp.where(diagonal, 1.0, 0.0)

    wide = jnp.concatenate([block, block], axis=1)

    def times(rows_of, stacked, by_rows):
        count = len(rows_of)
        if by_rows:
            o = mxu(jnp.concatenate([x for v in rows_of for x in split(v)], axis=0), stacked)
            o = [o[80 * k:80 * k + 40] + o[80 * k + 40:80 * k + 80] for k in range(count)]
        else:
            o = mxu(jnp.concatenate([jnp.concatenate(split(v), axis=1) for v in rows_of], axis=0),
                    jnp.concatenate([stacked, stacked], axis=0))
            o = [o[40 * k:40 * k + 40] for k in range(count)]
        return [x[:, 0:128] + x[:, 128:256] for x in o]

    def sweep(step, carry):
        for n in range(GROUPS):
            p, z = ps[n], zs[n]
            stacked = three_high(jnp.concatenate(split(p), axis=1), wide)
            pp, zp = times([p, z], stacked, BY_ROWS[0])
            zs[n] = 1.5 * z - 0.5 * zp
            q = 1.5 * p - 0.5 * pp
            ps[n] = 1.5 * q - 0.5 * times([q], stacked, BY_ROWS[1])[0]
        return carry

    lax.fori_loop(0, NS_ITERS - 1, sweep, 0, unroll=SWEEP_UNROLL)

    ones = jnp.where((block_of(iota((128, 128), 0)) == block) & (lane1 < 120), 1.0, 0.0).astype(F32)
    spreads, columns = [], []
    for n in range(GROUPS):
        z = zs[n]
        stacked = three_high(jnp.concatenate(split(ps[n]), axis=1), wide)
        z = 1.5 * z - 0.5 * times([z], stacked, BY_ROWS[2])[0]
        spreads.append(z / jnp.sqrt(tv[n:n + 1, :]))
        columns.append(jnp.concatenate(split(spreads[n] * gram[n, 40:41, :]), axis=1))
    partial = mxu(jnp.concatenate(columns, axis=0), jnp.concatenate([ones, ones], axis=0))
    transforms = []
    for n in range(GROUPS):
        centre = jnp.sum(spreads[n] * partial[40 * n:40 * n + 40], axis=0, keepdims=True)
        th, tl = split(spreads[n] + centre)
        transforms.append(jnp.concatenate([
            jnp.concatenate([th, th], axis=1), jnp.concatenate([tl, jnp.zeros_like(tl)], axis=1)], axis=0))

    patch = lax.rem(iota((1, 512), 1), 128) >> 3
    flat = y_ref.reshape(MEMBERS * 8, 128)
    for a in range(2):
        here = jnp.concatenate([pt[4 + 4 * a + r, 0:40, 0:128] for r in range(4)], axis=1)
        here = split(here)
        total = jnp.zeros((80, 512), F32)
        for g in range(6):
            n = 2 * g + a if g < 5 else 10
            ids = (3 * g, 3 * g + 1, 3 * g + 2) if g < 5 else (15, -1, -1) if a == 0 else (-1, 15, -1)
            pieces = []
            for v in here:
                pieces += [jnp.where(patch == c, v, 0.0) if c >= 0 else jnp.zeros((40, 512), F32) for c in ids]
                pieces.append(jnp.zeros((8, 512), F32))
            total = total + mxu(transforms[n], jnp.concatenate(pieces, axis=0))
        total = total[0:40] + total[40:80]
        for r in range(4):
            value = total[:, 128 * r:128 * r + 128] + pt[4 + 4 * a + r, 40:41, 0:128]
            for s in range(LEVELS):
                flat[pl.ds(80 * s + 4 * a + r, 8, stride=8), :] = value[8 * s:8 * s + 8]
                flat[pl.ds(80 * s + 64 + 4 * a + r, 2, stride=8), :] = value[32 + 2 * s:34 + 2 * s]
        done(a)


def compute_kernel(n_gx, n_gy, g_ref, a_ref, ob, y_ref, f0, f1, dif, wet, pt, hot, obs, slab, wc, *rest):
    grid = masks(n_gx, n_gy)
    weigh(ob, wc)
    aim(grid, a_ref, hot, obs, wc)
    assemble(grid, g_ref, a_ref, f0, dif, wet, (1,))
    forecast(f0, f1, dif, wet, pt, ((7, 10), 3), ((8, 10), 2))
    assemble(grid, g_ref, a_ref, f0, dif, wet, (0, 2))
    forecast(f0, f1, dif, wet, pt, ((1, 13), 6), ((2, 12), 6))
    analyse(grid, y_ref, lambda a: None, pt, hot, obs, slab, wc, *rest)


def scratch_of():
    return [
        pltpu.VMEM((20, 40, 256), F32), pltpu.VMEM((20, 40, 256), F32),
        pltpu.VMEM((20, 1, 256), F32), pltpu.VMEM((20, 1, 256), F32),
        pltpu.VMEM((16, 48, 256), F32), pltpu.VMEM((4, 512, 384), F32), pltpu.VMEM((8, 384), F32),
        pltpu.VMEM((4, 48, 384), F32), pltpu.VMEM((2, 16, 384), F32),
        pltpu.VMEM((12, 48, 128), F32), pltpu.VMEM((12, 128), F32), pltpu.VMEM((12, 128), F32),
        pltpu.VMEM((12, 40, 128), F32), pltpu.VMEM((12, 40, 128), F32)]


def solution(mesh):
    n_gx, n_gy = mesh.shape["gx"], mesh.shape["gy"]
    dma = pltpu.SemaphoreType.DMA

    def local(*args):
        def body(*refs):
            cycle_kernel(n_gx, n_gy, *refs)

        return pl.pallas_call(
            body, out_shape=jax.ShapeDtypeStruct((OWN, LEVELS, 8, 128), F32),
            in_specs=[pl.BlockSpec(memory_space=pl.ANY)] * 7, out_specs=pl.BlockSpec(memory_space=pltpu.VMEM),
            scratch_shapes=[pltpu.VMEM(a.shape, a.dtype) for a in args] + [
                pltpu.VMEM((LEVELS, 80, 128), F32), pltpu.VMEM((AUX, 128), F32), pltpu.VMEM((16, 256), F32),
                pltpu.VMEM((3, 3, LEVELS, 80, 128), F32), pltpu.VMEM((3, 3, AUX, 128), F32),
                pltpu.VMEM((LEVELS, OWN, 8, 128), F32)] + scratch_of() + [
                dma((3, LEVELS)), dma((3, LEVELS)), dma((3,)), dma((3,)),
                dma((2, 3, LEVELS + 1)), dma((2, 3, LEVELS + 1)), dma((7,)), dma((2, LEVELS)), dma((2, LEVELS))],
            compiler_params=pltpu.CompilerParams(collective_id=0, has_side_effects=True),
            name="cycle")(*args)

    return jax.shard_map(
        local,
        mesh=mesh,
        in_specs=(
            P("mem", None, "gx", "gy"),
            P(None, "gx", "gy"),
            P("gx", "gy"),
            P(None, None, "gx", "gy"),
            P(None, None, "gx", "gy"),
            P(None, None, "gx", "gy"),
            P(None, "gx", "gy"),
        ),
        out_specs=P("mem", None, "gx", "gy"),
        check_vma=False,
    )
```

```python
import jax
import jax.numpy as jnp
from jax import lax
from jax.experimental import pallas as pl
from jax.experimental.pallas import tpu as pltpu
from jax.sharding import PartitionSpec as P

MESH = pl.DeviceIdType.MESH
F32 = jnp.float32
NS_ITERS = 7
BY_ROWS = (False, False, False)
SWEEP_UNROLL = 5
FORECAST_UNROLL = 2
LEVELS = 4
OWN = 10
MEMBERS = 40
OBS = 16
MAIN = (64, 72, 20, 28, 36, 44, 0, 8)
REST = (60, 62, 52, 54, 56, 58, 16, 18)
AUX = 28
FLOW = (6, 7, 10, 11, 12, 13, 18, 19)
WET = (8, 9, 14, 15, 16, 17, 20, 21)
SEEN = (0, 22)
NEED = ((0, 60), (0, 80), (20, 60))
NEED_AUX = ((10, 18), (0, 28), (0, 18))


def neighbours(n_gx, n_gy):
    mem, gx, gy = lax.axis_index("mem"), lax.axis_index("gx"), lax.axis_index("gy")
    rows = (lax.rem(gx + n_gx - 1, n_gx), gx, lax.rem(gx + 1, n_gx))
    sides = (lax.rem(gy + n_gy - 1, n_gy), lax.rem(gy + 1, n_gy))
    there = [lax.rem(mem + o, LEVELS) for o in range(LEVELS)]
    back = [lax.rem(mem + LEVELS - o, LEVELS) for o in range(LEVELS)]
    return mem, gx, gy, rows, sides, there, back


def lay_out(x_ref, xs):
    flat = x_ref.reshape(OWN * LEVELS * 8, 128)
    for k in range(LEVELS):
        for r in range(8):
            xs[k, MAIN[r]:MAIN[r] + 8, :] = flat[pl.ds(k * 8 + r, 8, stride=32), :]
            xs[k, REST[r]:REST[r] + 2, :] = flat[pl.ds(256 + k * 8 + r, 2, stride=32), :]


def prepare(level, dif_ref, mask_ref, val_ref, var_ref, cell_ref, blk_ref, aux, ob):
    for rows, value in ((FLOW, dif_ref[level]), (WET, mask_ref[...].astype(F32))):
        for r in range(8):
            aux[rows[r]:rows[r] + 1, :] = value[r:r + 1]
    spread_out = jnp.where(iota((16, 256), 0) == iota((16, 256), 1) >> 4, 1.0, 0.0).astype(F32)
    kinds = [ref[level].astype(F32) for ref in (val_ref, var_ref, cell_ref)]
    stacked = jnp.concatenate([kinds[k][:, a, :] for a in range(2) for k in range(3)], axis=0)
    wide = lax.dot_general(stacked, spread_out, (((1,), (0,)), ((), ())), precision=lax.Precision.HIGHEST,
                           preferred_element_type=F32)
    mine = iota((16, 256), 0) == (iota((16, 256), 1) & 15)
    for n in range(6):
        row = jnp.sum(jnp.where(mine, wide[16 * n:16 * n + 16], 0.0), axis=0, keepdims=True)
        at = SEEN[n // 3] + 2 * (n % 3)
        aux[at:at + 1, :] = row[:, 0:128]
        aux[at + 1:at + 2, :] = row[:, 128:256]
    blocks = blk_ref[...].astype(F32)
    blocks = jnp.concatenate([blocks[:, a, :] for a in range(2)] + [jnp.zeros((6, 16), F32)], axis=0)
    ob[...] = mxu(blocks, spread_out)


def cycle_kernel(n_gx, n_gy, x_any, dif_any, mask_any, val_any, var_any, cell_any, blk_any, out_ref,
                 x_ref, dif_ref, mask_ref, val_ref, var_ref, cell_ref, blk_ref, xs, aux, ob, g_ref, a_ref, y_ref, *rest):
    scratch, (ssem, rsem, asem, arsem, fsem, frsem, lsem, bsem, brsem) = rest[:-9], rest[-9:]
    mem, gx, gy, rows, sides, there, back = neighbours(n_gx, n_gy)

    in_rows = (gx > 0, None, gx < n_gx - 1)
    in_sides = (gy > 0, gy < n_gy - 1)

    def when(*conditions):
        known = [c for c in conditions if c is not None]
        if not known:
            return lambda f: f()
        return pl.when(known[0] if len(known) == 1 else known[0] & known[1])

    barrier = pltpu.get_barrier_semaphore()
    count = LEVELS - 1
    for d in range(3):
        @when(in_rows[d])
        def _():
            for o in range(1, LEVELS) if d == 1 else (0,):
                pl.semaphore_signal(barrier, inc=1, device_id=(there[o], rows[d], gy), device_id_type=MESH)
        if d != 1:
            count = count + jnp.where(in_rows[d], 1, 0)
    for e in range(2):
        @when(in_sides[e])
        def _():
            pl.semaphore_signal(barrier, inc=1, device_id=(mem, gx, sides[e]), device_id_type=MESH)
        count = count + jnp.where(in_sides[e], 1, 0)

    loads = [pltpu.make_async_copy(src, dst, lsem.at[n]) for n, (src, dst) in enumerate((
        (x_any, x_ref), (dif_any, dif_ref), (mask_any, mask_ref), (val_any, val_ref), (var_any, var_ref),
        (cell_any, cell_ref), (blk_any, blk_ref)))]
    for load in loads:
        load.start()
    loads[0].wait()
    lay_out(x_ref, xs)
    f0, f1, dif, wet, pt, hot, obs, slab, wc = scratch[:9]
    grid = masks(n_gx, n_gy)
    pl.semaphore_wait(barrier, count)

    sends = []

    def start(copy, *conditions):
        when(*conditions)(copy.start)
        sends.append((copy, conditions))

    def forward(source, dg, slot, part, index):
        for e, side in enumerate(sides):
            h = 2 if e == 0 else 0
            dst = a_ref.at[h, dg, part] if slot is None else g_ref.at[h, dg, slot, part]
            start(pltpu.make_async_remote_copy(
                src_ref=source, dst_ref=dst, send_sem=fsem.at[e, dg, index], recv_sem=frsem.at[h // 2, dg, index],
                device_id=(mem, gx, side), device_id_type=MESH), in_rows[dg], in_sides[e])

    def scatter(o):
        start(pltpu.make_async_remote_copy(
            src_ref=xs.at[there[o]], dst_ref=g_ref.at[1, 1, mem], send_sem=ssem.at[1, o], recv_sem=rsem.at[1, o],
            device_id=(there[o], gx, gy), device_id_type=MESH))

    def halo(source, slot, o):
        for d in (0, 2):
            part = pl.ds(*NEED[2 - d])
            start(pltpu.make_async_remote_copy(
                src_ref=source.at[part], dst_ref=g_ref.at[1, 2 - d, slot, part],
                send_sem=ssem.at[d, o], recv_sem=rsem.at[2 - d, o],
                device_id=(mem, rows[d], gy), device_id_type=MESH), in_rows[d])

    def scatter_aux(d):
        part = pl.ds(*NEED_AUX[2 - d])
        start(pltpu.make_async_remote_copy(
            src_ref=aux.at[part], dst_ref=a_ref.at[1, 2 - d, part], send_sem=asem.at[d], recv_sem=arsem.at[2 - d],
            device_id=(mem, rows[d], gy), device_id_type=MESH), in_rows[d])

    for o in (2, 1, 3):
        scatter(o)
    halo(xs.at[mem], mem, 0)
    forward(xs.at[mem], 1, mem, pl.ds(0, 80), 0)
    for load in loads[1:]:
        load.wait()
    prepare(mem, dif_ref, mask_ref, val_ref, var_ref, cell_ref, blk_ref, aux, ob)
    for d in (0, 2):
        scatter_aux(d)
    forward(aux, 1, None, pl.ds(*NEED_AUX[1]), LEVELS)
    for dg in (0, 2):
        @when(~in_rows[dg])
        def _():
            for h in range(3):
                g_ref[h, dg] = jnp.zeros((LEVELS, 80, 128), F32)
                a_ref[h, dg] = jnp.ones((AUX, 128), F32)
    for h in (0, 2):
        @when(~in_sides[h // 2])
        def _():
            g_ref[h] = jnp.zeros((3, LEVELS, 80, 128), F32)
            a_ref[h] = jnp.ones((3, AUX, 128), F32)
    g_ref[1, 1, mem] = xs[mem]
    a_ref[1, 1] = aux[...]

    def arrival(dg, o):
        part = pl.ds(*NEED[dg])

        @when(in_rows[dg])
        def _():
            pltpu.make_async_remote_copy(
                src_ref=xs.at[0, part], dst_ref=g_ref.at[1, dg, back[o], part],
                send_sem=ssem.at[dg, o], recv_sem=rsem.at[dg, o],
                device_id=(mem, rows[dg], gy), device_id_type=MESH).wait_recv()
        if dg == 1:
            halo(g_ref.at[1, 1, back[o]], back[o], o)
        forward(g_ref.at[1, dg, back[o], part], dg, back[o], part, o)

    for o in (1, 3, 2):
        arrival(1, o)
    for dg in (0, 2):
        part = pl.ds(*NEED_AUX[dg])

        @when(in_rows[dg])
        def _():
            pltpu.make_async_remote_copy(
                src_ref=aux.at[part], dst_ref=a_ref.at[1, dg, part], send_sem=asem.at[dg], recv_sem=arsem.at[dg],
                device_id=(mem, rows[dg], gy), device_id_type=MESH).wait_recv()
        forward(a_ref.at[1, dg, part], dg, None, part, LEVELS)
    def passed_on(h, dg, chunks):
        @when(in_sides[h // 2], in_rows[dg])
        def _():
            for o in range(LEVELS) if chunks else ():
                part = pl.ds(*NEED[dg])
                pltpu.make_async_remote_copy(
                    src_ref=xs.at[0, part], dst_ref=g_ref.at[h, dg, back[o], part],
                    send_sem=fsem.at[0, dg, o], recv_sem=frsem.at[h // 2, dg, o],
                    device_id=(mem, gx, sides[0]), device_id_type=MESH).wait_recv()
            if not chunks:
                pltpu.make_async_remote_copy(
                    src_ref=aux.at[pl.ds(*NEED_AUX[dg])], dst_ref=a_ref.at[h, dg, pl.ds(*NEED_AUX[dg])],
                    send_sem=fsem.at[0, dg, LEVELS], recv_sem=frsem.at[h // 2, dg, LEVELS],
                    device_id=(mem, gx, sides[0]), device_id_type=MESH).wait_recv()

    weigh(ob, wc)
    for dg in (0, 2):
        arrival(dg, 0)
    for h in (0, 2):
        passed_on(h, 1, True)
        for dg in (1, 0, 2):
            passed_on(h, dg, False)
    assemble(grid, g_ref, a_ref, f0, dif, wet, (1,))
    forecast(f0, f1, dif, wet, pt, ((7, 10), 3), ((8, 10), 2))
    aim(grid, a_ref, hot, obs, wc)
    for o in (1, 3, 2):
        for dg in (0, 2):
            arrival(dg, o)
    for h in (0, 2):
        for dg in (0, 2):
            passed_on(h, dg, True)
    assemble(grid, g_ref, a_ref, f0, dif, wet, (0, 2))
    forecast(f0, f1, dif, wet, pt, ((1, 13), 6), ((2, 12), 6))
    def give_back(a):
        part = pl.ds(4 * a, 4)
        for o in (2, 1, 3):
            start(pltpu.make_async_remote_copy(
                src_ref=y_ref.at[there[o], :, part], dst_ref=out_ref.at[:, mem, part],
                send_sem=bsem.at[a, o], recv_sem=brsem.at[a, o],
                device_id=(there[o], gx, gy), device_id_type=MESH))

    analyse(grid, y_ref, give_back, pt, hot, obs, slab, wc, *scratch[9:])
    out_ref[:, mem] = y_ref[mem]
    for a in range(2):
        for o in range(1, LEVELS):
            part = pl.ds(4 * a, 4)
            pltpu.make_async_remote_copy(
                src_ref=y_ref.at[0, :, part], dst_ref=out_ref.at[:, back[o], part],
                send_sem=bsem.at[a, o], recv_sem=brsem.at[a, o],
                device_id=(there[o], gx, gy), device_id_type=MESH).wait_recv()
    for copy, conditions in sends:
        when(*conditions)(copy.wait_send)


def split(x):
    high = x.astype(jnp.bfloat16).astype(F32)
    return high, x - high


def mxu(a, b):
    return lax.dot_general(a, b, (((1,), (0,)), ((), ())), preferred_element_type=F32)


def mxu_nt(a, b):
    return lax.dot_general(a, b, (((1,), (1,)), ((), ())), preferred_element_type=F32)


def iota(shape, axis):
    return lax.broadcasted_iota(jnp.int32, shape, axis)


def block_of(lane):
    return jnp.where(lane < 40, 0, jnp.where(lane < 80, 1, jnp.where(lane < 120, 2, 3)))


def three_high(value, block):
    parts = [jnp.where(block == i, value, 0.0) for i in range(3)]
    return jnp.concatenate(parts + [jnp.zeros((8, value.shape[1]), F32)], axis=0)


def masks(n_gx, n_gy):
    gx, gy = lax.axis_index("gx"), lax.axis_index("gy")
    one = lambda c: jnp.where(c, 1.0, 0.0).astype(F32)
    lane1 = iota((1, 128), 1)
    in_grid = (one(gx > 0), jnp.float32(1.0), one(gx < n_gx - 1))
    return in_grid, jnp.where(lane1 < 64, one(gy < n_gy - 1), one(gy > 0)), lane1


def weigh(ob_ref, wc):
    third = lax.rem(iota((1, 384), 1) >> 4, 3)
    for a in range(2):
        for r in range(3):
            near = []
            for c in range(3):
                code = 3 * r + c
                taper = 1.0 if code == 4 else 0.5 if (r == 1 or c == 1) else 0.25
                chosen = jnp.zeros((1, 256), F32)
                for s in range(5):
                    blocks = ob_ref[5 * a + s:5 * a + s + 1, :]
                    chosen = chosen + jnp.where(blocks == code, taper, 0.0)
                chosen = jnp.concatenate([chosen, jnp.zeros((1, 128), F32)], axis=1)
                near.append(pltpu.roll(chosen, (16 * (c - 1)) % 384, 1) if c != 1 else chosen)
            for i in range(3):
                which = lax.rem(third + 4 - i, 3)
                wc[a, 3 * r + i:3 * r + i + 1, :] = jnp.where(
                    which == 0, near[0], jnp.where(which == 1, near[1], near[2]))


def assemble(grid, g_ref, a_ref, f0, dif, wet, groups):
    in_grid, beside, lane1 = grid

    def both(h_of, dg):
        own, side = h_of(1), jnp.where(lane1 < 64, h_of(2), h_of(0)) * (beside * in_grid[dg])
        return (own if dg == 1 else own * in_grid[dg]), side

    for t in range(20):
        dg, r = (0, t + 2) if t < 6 else (1, t - 6) if t < 14 else (2, t - 14)
        if dg not in groups:
            continue
        main, rest = MAIN[r], REST[r]
        for s in range(LEVELS):
            own, side = both(lambda h: g_ref[h, dg, s, main:main + 8, :], dg)
            f0[t, 8 * s:8 * s + 8, 0:128] = own
            f0[t, 8 * s:8 * s + 8, 128:256] = side
            own, side = both(lambda h: g_ref[h, dg, s, rest:rest + 2, :], dg)
            f0[t, 32 + 2 * s:34 + 2 * s, 0:128] = own
            f0[t, 32 + 2 * s:34 + 2 * s, 128:256] = side
        own, side = both(lambda h: a_ref[h, dg, FLOW[r]:FLOW[r] + 1, :], dg)
        dif[t, :, 0:128] = own
        dif[t, :, 128:256] = side
        own, side = both(lambda h: a_ref[h, dg, WET[r]:WET[r] + 1, :], dg)
        wet[t, :, 0:128] = own
        wet[t, :, 128:256] = side


def advance(src, dif, wet, t):
    c = src[t]
    around = src[t + 1] + src[t - 1]
    around = around + pltpu.roll(c, 255, 1) + pltpu.roll(c, 1, 1)
    return wet[t] * (c + dif[t] * (around - 4.0 * c))


def forecast(f0, f1, dif, wet, pt, first, second):
    def one(k, carry):
        for low in first[0]:
            f1[low + k] = advance(f0, dif, wet, low + k)
        return carry

    lax.fori_loop(0, first[1], one, 0, unroll=FORECAST_UNROLL)

    def two(k, carry):
        for low in second[0]:
            value = advance(f1, dif, wet, low + k)
            m = jnp.sum(value, axis=0, keepdims=True) / MEMBERS
            pt[low + k - 2, 0:40, :] = value - m
            pt[low + k - 2, 40:48, :] = jnp.where(iota((8, 256), 0) == 0, m, 0.0)
        return carry

    lax.fori_loop(0, second[1], two, 0, unroll=FORECAST_UNROLL)


def aim(grid, a_ref, hot, obs, wc):
    in_grid, beside, lane1 = grid
    lane2 = iota((1, 256), 1)
    for p in range(4):
        dg, a = ((0, 1), (1, 0), (1, 1), (2, 0))[p]

        def rows_of(kind):
            at = SEEN[a] + 2 * kind
            own = jnp.concatenate([a_ref[1, dg, at:at + 1, :], a_ref[1, dg, at + 1:at + 2, :]], axis=1)
            return own, jnp.where(lane1 < 64, a_ref[2, dg, at:at + 1, :], a_ref[0, dg, at + 1:at + 2, :])

        value, variance, cell = rows_of(0), rows_of(1), rows_of(2)
        for k, (lane, shift) in enumerate(((lane2, 0), (lane1, jnp.where(lane1 < 64, 0, 64)))):
            c = cell[k].astype(jnp.int32)
            target = (c >> 3) * 128 + ((lane >> 4) << 3) + (c & 7) + shift
            at, width = 256 * k, lane.shape[1]

            def fill(n, carry):
                top = pl.multiple_of(n * 64, 64)
                hot[p, pl.ds(top, 64), at:at + width] = jnp.where(
                    iota((64, width), 0) == target - n * 64, 1.0, 0.0).astype(F32)
                return carry

            lax.fori_loop(0, 8, fill, 0)
        obs[p:p + 1, :] = jnp.concatenate(value, axis=1)
        inside = jnp.concatenate([jnp.ones((1, 256), F32), beside], axis=1) * in_grid[dg]
        obs[4 + p:5 + p, :] = inside / jnp.concatenate(variance, axis=1)
    for a in range(2):
        for r in range(3):
            p = a + r
            rows = wc[a, 3 * r:3 * r + 3, :] * obs[4 + p:5 + p, :]
            wc[a, 3 * r:3 * r + 3, :] = pltpu.roll(rows, 80 * (p % 3), 1) if p % 3 else rows


GROUPS = 11


def analyse(grid, y_ref, done, pt, hot, obs, slab, wc, gram, tr, tv, ps, zs):
    lane1 = grid[2]

    for p in range(4):
        found = []
        for k, (low, high) in enumerate(((0, 256), (256, 384))):
            rows = jnp.concatenate([pt[4 * p + r, :, 128 * k:128 * k + 128] for r in range(4)], axis=1)
            both_parts = mxu(jnp.concatenate(split(rows), axis=0), hot[p, :, low:high])
            found.append(both_parts[0:48] + both_parts[48:96])
        whole = jnp.concatenate(found, axis=1)
        tail = jnp.where(iota((8, 384), 0) == 0, obs[p:p + 1, :] - whole[40:48], 0.0)
        whole = jnp.concatenate([whole[0:40], tail], axis=0)
        slab[p] = pltpu.roll(whole, 80 * (p % 3), 1) if p % 3 else whole

    lane2 = iota((1, 256), 1)
    part = jnp.where(lane2 < 80, 0, jnp.where(lane2 < 160, 1, jnp.where(lane2 < 240, 2, 3)))
    slot = (lane2 - 80 * part) >> 4
    block = block_of(lane1)
    diagonal = (lane1 - 40 * block == iota((40, 128), 0)) & (lane1 < 120)

    def keep(n, o):
        system = jnp.where(diagonal, 1.0, 0.0) + o[0:40] / (MEMBERS - 1.0)
        gram[n, 0:40, :] = system
        gram[n, 40:48, :] = o[40:48] / (MEMBERS - 1.0)
        tr[n:n + 1, :] = jnp.sum(jnp.where(diagonal, system, 0.0), axis=0, keepdims=True)

    last = []
    for g in range(6):
        turn = (16 - 48 * g) % 384

        def window(x):
            return pltpu.roll(x, turn, 1)[:, 0:256]

        parts = [window(slab[p]) for p in range(4)]
        for a in range(2):
            left = jnp.where(part == 0, parts[3 * a], jnp.where(part == 1, parts[1], parts[2]))
            weights = window(wc[a])
            right = []
            for i in range(3):
                w = jnp.zeros((1, 256), F32)
                for r in range(3):
                    w = jnp.where(part == (a + r) % 3, weights[3 * r + i:3 * r + i + 1], w)
                w = jnp.where((part < 3) & (slot >= i) & (slot <= i + 2), w, 0.0)
                right.append(left[0:40] * w)
            right.append(jnp.zeros((8, 256), F32))
            right = jnp.concatenate(right, axis=0)
            o = mxu_nt(jnp.concatenate(split(left), axis=0), jnp.concatenate(split(right), axis=0))
            o = o[0:48] + o[48:96]
            o = o[:, 0:128] + o[:, 128:256]
            if g < 5:
                keep(2 * g + a, o)
            else:
                last.append(o)
    keep(10, jnp.where(block == 0, last[0], jnp.where(block == 1, pltpu.roll(last[1], 40, 1), 0.0)))
    tr[11:12, :] = jnp.ones((1, 128), F32)

    rows = tr[...]
    sums = [jnp.sum(jnp.where(block == i, rows, 0.0), axis=1, keepdims=True) for i in range(3)]
    tv[...] = jnp.where(block == 0, sums[0], jnp.where(block == 1, sums[1], sums[2]))
    for n in range(GROUPS):
        ps[n] = gram[n, 0:40, :] / tv[n:n + 1, :]

    wide = jnp.concatenate([block, block], axis=1)

    def times(rows_of, stacked, by_rows):
        count = len(rows_of)
        if by_rows:
            o = mxu(jnp.concatenate([x for v in rows_of for x in split(v)], axis=0), stacked)
            o = [o[80 * k:80 * k + 40] + o[80 * k + 40:80 * k + 80] for k in range(count)]
        else:
            o = mxu(jnp.concatenate([jnp.concatenate(split(v), axis=1) for v in rows_of], axis=0),
                    jnp.concatenate([stacked, stacked], axis=0))
            o = [o[40 * k:40 * k + 40] for k in range(count)]
        return [x[:, 0:128] + x[:, 128:256] for x in o]

    for n in range(GROUPS):
        p = ps[n]
        stacked = three_high(jnp.concatenate(split(p), axis=1), wide)
        zs[n] = jnp.where(diagonal, 1.5, 0.0) - 0.5 * p
        q = 1.5 * p - 0.5 * times([p], stacked, BY_ROWS[0])[0]
        ps[n] = 1.5 * q - 0.5 * times([q], stacked, BY_ROWS[1])[0]

    def sweep(step, carry):
        for n in range(GROUPS):
            p, z = ps[n], zs[n]
            stacked = three_high(jnp.concatenate(split(p), axis=1), wide)
            pp, zp = times([p, z], stacked, BY_ROWS[0])
            zs[n] = 1.5 * z - 0.5 * zp
            q = 1.5 * p - 0.5 * pp
            ps[n] = 1.5 * q - 0.5 * times([q], stacked, BY_ROWS[1])[0]
        return carry

    lax.fori_loop(0, NS_ITERS - 2, sweep, 0, unroll=SWEEP_UNROLL)

    ones = jnp.where((block_of(iota((128, 128), 0)) == block) & (lane1 < 120), 1.0, 0.0).astype(F32)
    spreads, columns = [], []
    for n in range(GROUPS):
        z = zs[n]
        stacked = three_high(jnp.concatenate(split(ps[n]), axis=1), wide)
        z = 1.5 * z - 0.5 * times([z], stacked, BY_ROWS[2])[0]
        spreads.append(z / jnp.sqrt(tv[n:n + 1, :]))
        columns.append(jnp.concatenate(split(spreads[n] * gram[n, 40:41, :]), axis=1))
    partial = mxu(jnp.concatenate(columns, axis=0), jnp.concatenate([ones, ones], axis=0))
    transforms = []
    for n in range(GROUPS):
        centre = jnp.sum(spreads[n] * partial[40 * n:40 * n + 40], axis=0, keepdims=True)
        th, tl = split(spreads[n] + centre)
        transforms.append(jnp.concatenate([
            jnp.concatenate([th, th], axis=1), jnp.concatenate([tl, jnp.zeros_like(tl)], axis=1)], axis=0))

    patch = lax.rem(iota((1, 512), 1), 128) >> 3
    flat = y_ref.reshape(MEMBERS * 8, 128)
    for a in range(2):
        here = jnp.concatenate([pt[4 + 4 * a + r, 0:40, 0:128] for r in range(4)], axis=1)
        here = split(here)
        total = jnp.zeros((80, 512), F32)
        for g in range(6):
            n = 2 * g + a if g < 5 else 10
            ids = (3 * g, 3 * g + 1, 3 * g + 2) if g < 5 else (15, -1, -1) if a == 0 else (-1, 15, -1)
            pieces = []
            for v in here:
                pieces += [jnp.where(patch == c, v, 0.0) if c >= 0 else jnp.zeros((40, 512), F32) for c in ids]
                pieces.append(jnp.zeros((8, 512), F32))
            total = total + mxu(transforms[n], jnp.concatenate(pieces, axis=0))
        total = total[0:40] + total[40:80]
        for r in range(4):
            value = total[:, 128 * r:128 * r + 128] + pt[4 + 4 * a + r, 40:41, 0:128]
            for s in range(LEVELS):
                flat[pl.ds(80 * s + 4 * a + r, 8, stride=8), :] = value[8 * s:8 * s + 8]
                flat[pl.ds(80 * s + 64 + 4 * a + r, 2, stride=8), :] = value[32 + 2 * s:34 + 2 * s]
        done(a)


def compute_kernel(n_gx, n_gy, g_ref, a_ref, ob, y_ref, f0, f1, dif, wet, pt, hot, obs, slab, wc, *rest):
    grid = masks(n_gx, n_gy)
    weigh(ob, wc)
    aim(grid, a_ref, hot, obs, wc)
    assemble(grid, g_ref, a_ref, f0, dif, wet, (1,))
    forecast(f0, f1, dif, wet, pt, ((7, 10), 3), ((8, 10), 2))
    assemble(grid, g_ref, a_ref, f0, dif, wet, (0, 2))
    forecast(f0, f1, dif, wet, pt, ((1, 13), 6), ((2, 12), 6))
    analyse(grid, y_ref, lambda a: None, pt, hot, obs, slab, wc, *rest)


def scratch_of():
    return [
        pltpu.VMEM((20, 40, 256), F32), pltpu.VMEM((20, 40, 256), F32),
        pltpu.VMEM((20, 1, 256), F32), pltpu.VMEM((20, 1, 256), F32),
        pltpu.VMEM((16, 48, 256), F32), pltpu.VMEM((4, 512, 384), F32), pltpu.VMEM((8, 384), F32),
        pltpu.VMEM((4, 48, 384), F32), pltpu.VMEM((2, 16, 384), F32),
        pltpu.VMEM((12, 48, 128), F32), pltpu.VMEM((12, 128), F32), pltpu.VMEM((12, 128), F32),
        pltpu.VMEM((12, 40, 128), F32), pltpu.VMEM((12, 40, 128), F32)]


def solution(mesh):
    n_gx, n_gy = mesh.shape["gx"], mesh.shape["gy"]
    dma = pltpu.SemaphoreType.DMA

    def local(*args):
        def body(*refs):
            cycle_kernel(n_gx, n_gy, *refs)

        return pl.pallas_call(
            body, out_shape=jax.ShapeDtypeStruct((OWN, LEVELS, 8, 128), F32),
            in_specs=[pl.BlockSpec(memory_space=pl.ANY)] * 7, out_specs=pl.BlockSpec(memory_space=pltpu.VMEM),
            scratch_shapes=[pltpu.VMEM(a.shape, a.dtype) for a in args] + [
                pltpu.VMEM((LEVELS, 80, 128), F32), pltpu.VMEM((AUX, 128), F32), pltpu.VMEM((16, 256), F32),
                pltpu.VMEM((3, 3, LEVELS, 80, 128), F32), pltpu.VMEM((3, 3, AUX, 128), F32),
                pltpu.VMEM((LEVELS, OWN, 8, 128), F32)] + scratch_of() + [
                dma((3, LEVELS)), dma((3, LEVELS)), dma((3,)), dma((3,)),
                dma((2, 3, LEVELS + 1)), dma((2, 3, LEVELS + 1)), dma((7,)), dma((2, LEVELS)), dma((2, LEVELS))],
            compiler_params=pltpu.CompilerParams(collective_id=0, has_side_effects=True),
            name="cycle")(*args)

    return jax.shard_map(
        local,
        mesh=mesh,
        in_specs=(
            P("mem", None, "gx", "gy"),
            P(None, "gx", "gy"),
            P("gx", "gy"),
            P(None, None, "gx", "gy"),
            P(None, None, "gx", "gy"),
            P(None, None, "gx", "gy"),
            P(None, "gx", "gy"),
        ),
        out_specs=P("mem", None, "gx", "gy"),
        check_vma=False,
    )
```
